128 devices in a mesh: teacher: 8 (over z_hi, y), student: 16 (over z_lo, x, core).
Axes of the slice: x: 4, y: 4, z: 4 (z_hi: 2, z_lo: 2; z = z_hi * 2 + z_lo), core: 2. Of those that a mesh axis runs over, the one named last changes fastest.
Arguments:
- teacher_in: bfloat16 [16384, 8192], P('student', 'teacher')
- teacher_attn: bfloat16 [16384, 4096], P('student', 'teacher'), may hold values from -6 to 6
- teacher_out_proj: bfloat16 [4096, 8192], P('student', 'teacher'), may hold values from -0.09375 to 0.09375
- teacher_gain: bfloat16 [8192], P('teacher'), may hold values from 0.099609375 to 1.8984375
- projection: bfloat16 [8192, 4096], P('teacher', 'student'), may hold values from -0.0625 to 0.0625
- student_in: bfloat16 [16384, 4096], P('student', 'teacher')
- student_attn: bfloat16 [16384, 2048], P('student', 'teacher'), may hold values from -6 to 6
- student_out_proj: bfloat16 [2048, 4096], P('student', 'teacher'), may hold values from -0.125 to 0.125
- student_gain: bfloat16 [4096], P('teacher'), may hold values from 0.099609375 to 1.8984375
- token_ids: int32 [16384], P('student'), may hold values from 0 to 128004, as said below
- row_order: int32 [16384], replicated, may hold values from 0 to 16383, as said below
Outputs:
- grad_weight: float32 [2048, 4096], P('student', 'teacher')
- grad_gain: float32 [4096], P('teacher')
The draws below stay inside these ranges and needn't reach their ends.
Inputs may be any that keep to these rules, and one draw needn't show every extreme that they name: `token_ids`: within each sequence of 1024 consecutive rows the rows holding 128004 form the sequence's tail, after at least 256 other rows; no other row holds 128004. `row_order`: A permutation of the 16384 rows. For student block k and teacher block b (blocks of 1024 rows), the entries k * 1024 + b * 64 to k * 1024 + (b + 1) * 64 - 1 name rows of teacher block b.
All inputs are finite; a program needn't handle non-finite values.
Results may differ from the reference program's by a relative error of at most 0.02.
Values may be sent and summed in bfloat16 or wider, within the bound.
A program may use at most 128 MiB of HBM per device.

```python
import jax
import jax.numpy as jnp
from jax import lax

DT = 8192
DS = 4096
HEAD = 128
HT = 32
HS = 16
SEQ = 1024
PAD_ID = 128004
GROUP_ROWS = 1024
TOKENS = 16384
PIECE = 64
N_TEACHER = 8


def scaled_rows(key, row_count, column_count):
    first_key, second_key = jax.random.split(key, 2)
    normal_base = jax.random.normal(first_key, (row_count, column_count), jnp.float32)
    column_ramp = jnp.arange(column_count, dtype=jnp.float32) / column_count
    jitter = jnp.exp(0.3 * jax.random.normal(second_key, (column_count,), jnp.float32))
    column_scale = jnp.exp(jnp.log(5.0) * column_ramp) * jitter
    return normal_base * column_scale[None, :]


def draw_teacher_in(key, part):
    return scaled_rows(jax.random.fold_in(key, 11), TOKENS, DT).astype(jnp.bfloat16)


def draw_student_in(key, part):
    return scaled_rows(jax.random.fold_in(key, 23), TOKENS, DS).astype(jnp.bfloat16)


def draw_token_ids(key, part):
    first_key, second_key = jax.random.split(jax.random.fold_in(key, 37))
    sequence_count = TOKENS // SEQ
    live_len = jax.random.randint(first_key, (sequence_count, 1), SEQ // 4, SEQ + 1)
    word_ids = jax.random.randint(second_key, (sequence_count, SEQ), 0, PAD_ID)
    position = jnp.arange(SEQ)[None, :]
    return jnp.where(position < live_len, word_ids, PAD_ID).reshape(TOKENS).astype(jnp.int32)


def draw_row_order(key, part):
    block_count = TOKENS // GROUP_ROWS
    block_keys = jax.random.split(jax.random.fold_in(key, 41), block_count)
    shuffled = jax.vmap(lambda one_key: jax.random.permutation(one_key, GROUP_ROWS))(block_keys)
    shuffled = shuffled + (jnp.arange(block_count) * GROUP_ROWS)[:, None]
    shuffled = shuffled.reshape(block_count, block_count, PIECE)
    return jnp.transpose(shuffled, (1, 0, 2)).reshape(TOKENS).astype(jnp.int32)


def strengthened(array, own_key, source, target, parts, factor):
    def block_of(axis_at):
        return (jnp.arange(array.shape[axis_at]) // (array.shape[axis_at] // parts)).reshape((-1,) + (1,) * (array.ndim - 1 - axis_at))

    one_side = jax.random.permutation(own_key, parts)[block_of(target)]
    second = (block_of(target) + parts // 2) % parts
    return jnp.where((block_of(source) == one_side) | (block_of(source) == second), factor * array, array)


def level_of(rng, extent, cuts, least, largest):
    gain, own = 1.0, jax.random.fold_in(rng, 6)
    for dim, blocks in cuts:
        heights = jnp.exp(jax.random.uniform(jax.random.fold_in(own, dim), (blocks,), jnp.float32, least / len(cuts), largest / len(cuts)))
        gain = gain * jnp.repeat(heights, extent[dim] // blocks).reshape([-1 if axis == dim else 1 for axis in range(len(extent))])
    return gain


def normal_values(stream_key, shape, width, bound, pieces=(), kind=jnp.bfloat16):
    result = width * jax.random.normal(stream_key, shape, jnp.float32)
    if pieces:
        result = result * level_of(stream_key, shape, pieces, -0.22, 0.18)
    return jnp.clip(result, -bound, bound).astype(kind)


def gaussian_with(stream_key, shape, scale, bound, pieces, heavy, held_as=jnp.bfloat16):
    values = scale * jax.random.normal(stream_key, shape, jnp.float32)
    if pieces:
        values = values * level_of(stream_key, shape, pieces, -0.22, 0.18)
    return jnp.clip(strengthened(values, jax.random.fold_in(stream_key, 3), *heavy), -bound, bound).astype(held_as)


def setup_inputs(seed: int = 0) -> dict:
    key_list = jax.random.split(jax.random.key(seed), 12)
    return {
        "teacher_in": draw_teacher_in(jax.random.fold_in(key_list[11], 71), 0),
        "teacher_attn": normal_values(key_list[1], (TOKENS, HT * HEAD), 1.0, 6.0, ((0, 16), (1, 8))),
        "teacher_out_proj": normal_values(key_list[2], (HT * HEAD, DT), (HT * HEAD) ** -0.5, 0.09375, ((0, 16), (1, 8))),
        "teacher_gain": jnp.clip(1.0 + 0.18 * jax.random.normal(key_list[3], (DT,), jnp.float32), 0.099609375, 1.8984375).astype(jnp.bfloat16),
        "projection": normal_values(key_list[4], (DT, DS), DT ** -0.5, 0.0625, ((0, 8), (1, 16))),
        "student_in": draw_student_in(jax.random.fold_in(key_list[11], 71), 0),
        "student_attn": gaussian_with(key_list[6], (TOKENS, HS * HEAD), 1.0, 6.0, ((0, 16), (1, 8)), (0, 1, 16, 2.0)),
        "student_out_proj": normal_values(key_list[7], (HS * HEAD, DS), (HS * HEAD) ** -0.5, 0.125, ((0, 16), (1, 8))),
        "student_gain": jnp.clip(1.0 + 0.18 * jax.random.normal(key_list[8], (DS,), jnp.float32), 0.099609375, 1.8984375).astype(jnp.bfloat16),
        "token_ids": draw_token_ids(jax.random.fold_in(key_list[11], 71), 0),
        "row_order": draw_row_order(jax.random.fold_in(key_list[11], 71), 0),
    }


epsilon = 1e-05

def reference(teacher_in, teacher_attn, teacher_out_proj, teacher_gain, projection, student_in, student_attn, student_out_proj, student_gain, token_ids, row_order):
    residual = teacher_in.astype(jnp.float32) + jnp.dot(teacher_attn, teacher_out_proj, preferred_element_type=jnp.float32)
    teacher_scale = lax.rsqrt(lax.optimization_barrier(jnp.mean(residual * residual, axis=1, keepdims=True)) + epsilon)
    hidden = (residual * teacher_scale * teacher_gain.astype(jnp.float32)).astype(jnp.bfloat16)
    block_width = DT // N_TEACHER
    summed = jnp.zeros((TOKENS, DS), jnp.float32)
    for block in range(N_TEACHER):
        lower = block * block_width
        partial_term = jnp.dot(hidden[:, lower:lower + block_width], projection[lower:lower + block_width], preferred_element_type=jnp.float32)
        rounded = lax.optimization_barrier(partial_term.astype(jnp.bfloat16))
        summed = summed + rounded.astype(jnp.float32)
    target = summed.astype(jnp.bfloat16)
    live_rows = jnp.where(token_ids != PAD_ID, 1.0, 0.0).astype(jnp.float32)
    target_s = jnp.take(target, row_order, axis=0).astype(jnp.float32)
    live_s = jnp.take(live_rows, row_order, axis=0)
    student_res = student_in.astype(jnp.float32) + jnp.dot(student_attn, student_out_proj, preferred_element_type=jnp.float32)
    student_scale = lax.rsqrt(lax.optimization_barrier(jnp.mean(student_res * student_res, axis=1, keepdims=True)) + epsilon)
    normed = student_res * student_scale
    gain_values = student_gain.astype(jnp.float32)
    distance = normed * gain_values - target_s
    loss_weight = 1.0 / jnp.sqrt(jnp.float32(TOKENS))
    grad_out = distance * (live_s * loss_weight)[:, None]
    grad_gain = lax.optimization_barrier(jnp.sum(grad_out * normed, axis=0))
    grad_norm = grad_out * gain_values
    inner = lax.optimization_barrier(jnp.mean(grad_norm * normed, axis=1, keepdims=True))
    grad_res = (student_scale * (grad_norm - normed * inner)).astype(jnp.bfloat16)
    grad_weight = jnp.dot(student_attn.T, grad_res, preferred_element_type=jnp.float32)
    return (grad_weight, grad_gain)
```

```python
import math

import jax
import jax.numpy as jnp
from jax import lax
from jax.experimental import pallas as pl
from jax.experimental.pallas import tpu as pltpu
from jax.sharding import PartitionSpec as P

DT = 8192
DS = 4096
PAD_ID = 128004
epsilon = 1e-05

BF = jnp.bfloat16
F32 = jnp.float32
SLOTS = 160


def div(a, b):
    return lax.div(a, jnp.int32(b))


def rem(a, b):
    return lax.rem(a, jnp.int32(b))


class Place:
    def __init__(self):
        t = lax.axis_index("teacher")
        s = lax.axis_index("student")
        self.t, self.s = t, s
        self.zh, self.y = div(t, 4), rem(t, 4)
        self.zl, self.x, self.core = div(s, 8), rem(div(s, 2), 4), rem(s, 2)
        self.z = self.zh * 2 + self.zl

    def dev(self, dz=0, dy=0, dx=0, dc=0):
        t, s = self.index(dz, dy, dx, dc)
        return {"teacher": t, "student": s}

    def index(self, dz=0, dy=0, dx=0, dc=0):
        z, y, x, c = self.z, self.y, self.x, self.core
        if dz:
            z = rem(z + (dz % 4), 4)
        if dy:
            y = rem(y + (dy % 4), 4)
        if dx:
            x = rem(x + (dx % 4), 4)
        if dc:
            c = 1 - c
        return div(z, 2) * 4 + y, rem(z, 2) * 8 + x * 2 + c


class Net:
    def __init__(self, send, recv):
        self.send, self.recv, self.n, self.open = send, recv, 0, []

    def copy(self, src, dst, device):
        c = pltpu.make_async_remote_copy(
            src_ref=src,
            dst_ref=dst,
            send_sem=self.send.at[self.n],
            recv_sem=self.recv.at[self.n],
            device_id=device,
            device_id_type=pl.DeviceIdType.MESH,
        )
        self.n += 1
        c.start()
        self.open.append(c)
        return c

    def sent(self, copies):
        for c in copies:
            c.wait_send()
        gone = {id(c) for c in copies}
        self.open = [c for c in self.open if id(c) not in gone]

    def finish(self):
        for c in self.open:
            c.wait_send()
        self.open = []


def got(*copies):
    for c in copies:
        c.wait_recv()


def gather_kernel(
    tin, tattn, tw, tgain, proj, sin, sattn, su,
    target_out, sq_out, sres_out, attn_out, ssq_out,
    bufA, bufC, bufW, bufP, bufU, tinv, sinv, hid,
    tmpA, tmpC, tmpE, r1, r2, r3, zs,
    send, recv, local,
):
    p = Place()
    up, down = {"dy": 1}, {"dy": -1}
    barrier = pltpu.get_barrier_semaphore()
    near = [dict(dy=1), dict(dy=-1), dict(dz=1), dict(dz=-1), dict(dx=1), dict(dx=-1), dict(dc=1)]
    for n in near:
        pl.semaphore_signal(barrier, inc=1, device_id=p.dev(**n), device_id_type=pl.DeviceIdType.MESH)
    pl.semaphore_wait(barrier, len(near))
    net = Net(send, recv)

    A = (tattn, bufA, tmpA, 512)
    C = (sattn, bufC, tmpC, 512)
    W = (tw, bufW, 128)
    Q = (proj, bufP, 512)
    U = (su, bufU, 64)

    def own(arr, h):
        half = arr[-1]
        return arr[0].at[pl.ds(h * half, half), :]

    def slot(arr, i, h):
        half = arr[-1]
        return arr[1].at[i, pl.ds(h * half, half), :]

    tp = p.index(dz=2)[0]
    zpart = {"teacher": p.t, "student": rem(p.s + 8, 16)}
    sp = rem(p.s + 8, 16)
    sib = p.dev(dc=1)
    sib_index = p.index(dc=1)[1]
    locals_ = []

    def bring(src, dst):
        c = pltpu.make_async_copy(src, dst, local.at[len(locals_)])
        c.start()
        locals_.append(c)
        return c

    def t_own(arr):
        ups = [net.copy(own(arr, h), slot(arr, p.t, h), p.dev(dy=1)) for h in (0, 1)]
        downs = [net.copy(own(arr, h), slot(arr, p.t, h), p.dev(dy=-1)) for h in (1, 0)][::-1]
        return ups, downs

    def t_hop1(arr):
        return [
            net.copy(own(arr, 0), arr[2].at[0], p.dev(dz=1)),
            net.copy(own(arr, 1), arr[2].at[1], p.dev(dz=-1)),
        ]

    def t_hop2(arr, hop1):
        got(hop1[0])
        a = net.copy(arr[2].at[0], slot(arr, p.index(dz=-1)[0], 0), p.dev(dz=1))
        got(hop1[1])
        b = net.copy(arr[2].at[1], slot(arr, p.index(dz=1)[0], 1), p.dev(dz=-1))
        return [a, b]

    def t_forward(arr, ups, downs, dz):
        got(ups[0])
        a = net.copy(slot(arr, p.index(dz=dz, dy=-1)[0], 0), slot(arr, p.index(dz=dz, dy=-1)[0], 0), p.dev(dy=1))
        got(downs[1])
        b = net.copy(slot(arr, p.index(dz=dz, dy=1)[0], 1), slot(arr, p.index(dz=dz, dy=1)[0], 1), p.dev(dy=-1))
        return [a, b]

    def t_partner(arr, hop2):
        got(*hop2)
        ups = [net.copy(slot(arr, tp, h), slot(arr, tp, h), p.dev(dy=1)) for h in (0, 1)]
        downs = [net.copy(slot(arr, tp, h), slot(arr, tp, h), p.dev(dy=-1)) for h in (1, 0)][::-1]
        return ups, downs

    def s_own(arr):
        ups = [net.copy(own(arr, h), slot(arr, p.s, h), p.dev(dx=1)) for h in (0, 1)]
        downs = [net.copy(own(arr, h), slot(arr, p.s, h), p.dev(dx=-1)) for h in (1, 0)][::-1]
        return ups, downs

    def s_side(arr):
        return net.copy(arr[0], arr[1].at[p.s], zpart)

    def s_partner(arr, side):
        got(side)
        ups = [net.copy(slot(arr, sp, h), slot(arr, sp, h), p.dev(dx=1)) for h in (0, 1)]
        downs = [net.copy(slot(arr, sp, h), slot(arr, sp, h), p.dev(dx=-1)) for h in (1, 0)][::-1]
        return ups, downs

    def s_index(dx, other):
        i = p.index(dx=dx)[1]
        return rem(i + 8, 16) if other else i

    def s_forward(arr, ups, downs, other):
        got(ups[0])
        i = s_index(-1, other)
        a = net.copy(slot(arr, i, 0), slot(arr, i, 0), p.dev(dx=1))
        got(downs[1])
        j = s_index(1, other)
        b = net.copy(slot(arr, j, 1), slot(arr, j, 1), p.dev(dx=-1))
        return [a, b]

    def share(arr, i):
        return net.copy(arr[1].at[i], arr[1].at[i], sib)

    ssides, sowns, shared = {}, {}, []
    aown = t_own(A)
    ahop1 = t_hop1(A)
    for n, arr in (("W", W), ("Q", Q)):
        sowns[n] = s_own(arr)
        ssides[n] = s_side(arr)
        shared.append(net.copy(arr[0], arr[1].at[p.s], sib))
    bring(tattn, bufA.at[p.t])
    bring(tw, bufW.at[p.s])
    bring(proj, bufP.at[p.s])
    bring(tin, tinv)
    bring(sattn, bufC.at[p.t])
    bring(su, bufU.at[p.s])
    bring(sin, sinv)
    cown = t_own(C)

    ahop2 = t_hop2(A, ahop1)
    chop1 = t_hop1(C)
    sowns["U"] = s_own(U)
    ssides["U"] = s_side(U)
    shared.append(net.copy(U[0], U[1].at[p.s], sib))
    S = (("W", W), ("Q", Q), ("U", U))
    sfwd, sfwd2, sparts = {}, {}, {}
    for n, arr in S[:2]:
        sfwd[n] = s_forward(arr, *sowns[n], False)
    afwd = t_forward(A, *aown, 0)
    for n, arr in S[:2]:
        sparts[n] = s_partner(arr, ssides[n])
    apart = t_partner(A, ahop2)
    chop2 = t_hop2(C, chop1)
    for n, arr in S[:2]:
        got(sowns[n][0][1], sowns[n][1][0])
        shared.append(share(arr, sp))
        shared.append(share(arr, s_index(-1, False)))
        shared.append(share(arr, s_index(1, False)))
    sfwd["U"] = s_forward(U, *sowns["U"], False)
    sparts["U"] = s_partner(U, ssides["U"])
    for n, arr in S[:2]:
        sfwd2[n] = s_forward(arr, *sparts[n], True)
    afwd2 = t_forward(A, *apart, 2)
    cfwd = t_forward(C, *cown, 0)
    cpart = t_partner(C, chop2)
    for n, arr in S[:2]:
        got(*sfwd[n], sparts[n][0][1], sparts[n][1][0])
        shared.append(share(arr, s_index(2, False)))
        shared.append(share(arr, s_index(-1, True)))
        shared.append(share(arr, s_index(1, True)))
    sfwd2["U"] = s_forward(U, *sparts["U"], True)
    for n, arr in S[:2]:
        got(*sfwd2[n])
        shared.append(share(arr, s_index(2, True)))
    got(sowns["U"][0][1], sowns["U"][1][0], sparts["U"][0][1], sparts["U"][1][0], *sfwd["U"])
    ushared = [
        share(U, sp),
        share(U, s_index(-1, False)),
        share(U, s_index(1, False)),
        share(U, s_index(2, False)),
        share(U, s_index(-1, True)),
        share(U, s_index(1, True)),
    ]
    got(aown[0][1], aown[1][0], *afwd, apart[0][1], apart[1][0], *afwd2)
    got(*shared)
    for c in locals_:
        c.wait()

    sq_out[...] = jnp.zeros_like(sq_out)

    def first(i, carry):
        rows = pl.ds(pl.multiple_of(div(i, 2) * 512, 512), 512)
        cols = pl.ds(pl.multiple_of(rem(i, 2) * 512, 512), 512)
        acc = tinv[rows, cols].astype(F32)
        for t in range(8):
            w = bufW[2 * t : 2 * t + 2, :, cols].reshape(512, 512)
            acc = acc + jnp.dot(bufA[t, rows, :], w, preferred_element_type=F32)
        square = acc * acc
        sq_out[rows, :] += square[:, 0:128] + square[:, 128:256] + square[:, 256:384] + square[:, 384:512]
        hid[rows, cols] = (acc * tgain[:, cols].astype(F32)).astype(BF)
        return carry

    lax.fori_loop(0, 2, first, 0)
    cfwd2 = t_forward(C, *cpart, 2)
    lax.fori_loop(2, 4, first, 0)
    net.sent([*aown[0], *aown[1], *ahop1, *ahop2, *afwd, *apart[0], *apart[1], *afwd2])

    def project(k):
        def step(i, carry):
            rows = pl.ds(pl.multiple_of(i * 512, 512), 512)
            h = hid[rows, :]
            bufA[k, rows, 0:256] = jnp.dot(h, bufP[2 * k], preferred_element_type=F32).astype(BF)
            bufA[k, rows, 256:512] = jnp.dot(h, bufP[2 * k + 1], preferred_element_type=F32).astype(BF)
            return carry

        lax.fori_loop(0, 2, step, 0)

    def block(far, dy):
        zh = 1 - p.zh if far else p.zh
        y = rem(p.y + (dy % 4), 4)
        return zh * 4 + y

    lo, hi = pl.ds(0, 512), pl.ds(512, 512)

    def opening(n, far):
        k = block(far, 2)
        project(k)
        return (
            net.copy(bufA.at[k, lo, :], r1.at[n, 0], p.dev(dy=1)),
            net.copy(bufA.at[k, hi, :], r1.at[n, 1], p.dev(dy=-1)),
        )

    def plain(n, far):
        ku, kd = block(far, 1), block(far, -1)
        project(ku)
        u = net.copy(bufA.at[ku, hi, :], r2.at[n, 0, hi, :], p.dev(dy=1))
        project(kd)
        d = net.copy(bufA.at[kd, lo, :], r2.at[n, 1, lo, :], p.dev(dy=-1))
        return u, d

    def added(n, far, opened):
        ku, kd = block(far, 1), block(far, -1)

        def add(k, base, j):
            def step(i, carry):
                at = pl.ds(pl.multiple_of(i * 128, 128), 128)
                rows = pl.ds(pl.multiple_of(base + i * 128, 128), 128)
                bufA[k, rows, :] = (bufA[k, rows, :].astype(F32) + r1[n, j, at, :].astype(F32)).astype(BF)
                return carry

            lax.fori_loop(0, 4, step, 0)

        got(opened[0])
        add(ku, 0, 0)
        u = net.copy(bufA.at[ku, lo, :], r2.at[n, 0, lo, :], p.dev(dy=1))
        got(opened[1])
        add(kd, 512, 1)
        d = net.copy(bufA.at[kd, hi, :], r2.at[n, 1, hi, :], p.dev(dy=-1))
        return u, d

    open_far = opening(0, True)
    plain_far = plain(0, True)
    open_near = opening(1, False)
    added_far = added(0, True, open_far)
    plain_near = plain(1, False)
    added_near = added(1, False, open_near)
    k_far, k_near = block(True, 0), block(False, 0)
    project(k_far)
    project(k_near)

    got(cown[0][1], cown[1][0], *cfwd, cpart[0][1], cpart[1][0], *cfwd2)
    got(*sfwd2["U"])
    ushared.append(share(U, s_index(2, True)))
    got(*ushared)
    outs = []
    for t in range(8):
        c = pltpu.make_async_copy(
            bufC.at[t], attn_out.at[:, pl.ds(t * 256, 256)], local.at[len(locals_) + t]
        )
        c.start()
        outs.append(c)

    def student(i, carry):
        rows = pl.ds(pl.multiple_of(i * 512, 512), 512)
        acc = sinv[rows, :].astype(F32)
        for t in range(8):
            w = bufU[2 * t : 2 * t + 2].reshape(256, 512)
            acc = acc + jnp.dot(bufC[t, rows, :], w, preferred_element_type=F32)
        square = acc * acc
        ssq_out[rows, :] = square[:, 0:128] + square[:, 128:256] + square[:, 256:384] + square[:, 384:512]
        sres_out[rows, :] = acc
        return carry

    lax.fori_loop(0, 2, student, 0)

    def three(n, k, base, i):
        at = pl.ds(pl.multiple_of(base + i * 128, 128), 128)
        return at, (
            bufA[k, at, :].astype(F32) + r2[n, 0, at, :].astype(F32) + r2[n, 1, at, :].astype(F32)
        )

    got(*plain_far, *added_far)

    def far_sum(i, carry):
        at, total = three(0, k_far, 0, i)
        zs[at, :] = total.astype(BF)
        return carry

    lax.fori_loop(0, 8, far_sum, 0)
    hop1 = (
        net.copy(zs.at[lo, :], tmpE.at[0], p.dev(dz=1)),
        net.copy(zs.at[hi, :], tmpE.at[1], p.dev(dz=-1)),
    )
    got(hop1[0])
    h2a = net.copy(tmpE.at[0], r3.at[lo, :], p.dev(dz=1))
    got(hop1[1])
    h2b = net.copy(tmpE.at[1], r3.at[hi, :], p.dev(dz=-1))
    got(*plain_near, *added_near)
    got(h2a, h2b)

    def near_sum(i, carry):
        at, total = three(1, k_near, 0, i)
        target_out[at, :] = (total + r3[at, :].astype(F32)).astype(BF)
        return carry

    lax.fori_loop(0, 8, near_sum, 0)
    for c in outs:
        c.wait()
    net.finish()


def gathered(tin, tattn, tw, tgain, proj, sin, sattn, su):
    anywhere = pl.BlockSpec(memory_space=pl.ANY)
    vmem = pl.BlockSpec(memory_space=pltpu.VMEM)
    V = pltpu.VMEM
    return pl.pallas_call(
        gather_kernel,
        out_shape=(
            jax.ShapeDtypeStruct((1024, 512), BF),
            jax.ShapeDtypeStruct((1024, 128), F32),
            jax.ShapeDtypeStruct((1024, 512), F32),
            jax.ShapeDtypeStruct((1024, 2048), BF),
            jax.ShapeDtypeStruct((1024, 128), F32),
        ),
        in_specs=[anywhere, anywhere, anywhere, vmem, anywhere, anywhere, anywhere, anywhere],
        out_specs=(vmem, vmem, vmem, anywhere, vmem),
        scratch_shapes=[
            V((8, 1024, 512), BF),
            V((8, 1024, 256), BF),
            V((16, 256, 1024), BF),
            V((16, 1024, 256), BF),
            V((16, 128, 512), BF),
            V((1024, 1024), BF),
            V((1024, 512), BF),
            V((1024, 1024), BF),
            V((2, 512, 512), BF),
            V((2, 512, 256), BF),
            V((2, 512, 512), BF),
            V((2, 2, 512, 512), BF),
            V((2, 2, 1024, 512), BF),
            V((1024, 512), BF),
            V((1024, 512), BF),
            pltpu.SemaphoreType.DMA((SLOTS,)),
            pltpu.SemaphoreType.DMA((SLOTS,)),
            pltpu.SemaphoreType.DMA((16,)),
        ],
        compiler_params=pltpu.CompilerParams(
            collective_id=0, has_side_effects=True, vmem_limit_bytes=67043328
        ),
        name="gathered",
    )(tin, tattn, tw, tgain.reshape(1, -1), proj, sin, sattn, su)


def sent_to_all(array, axis):
    peers = lax.axis_size(axis)
    return lax.all_to_all(
        jnp.broadcast_to(array[None], (peers, *array.shape)), axis, 0, 0, tiled=True
    )


def of_everyone(array, axis):
    return jnp.sum(sent_to_all(array, axis), axis=0)


def shards(tin, tattn, tw, tgain, proj, sin, sattn, su, sgain, token_ids, row_order):
    s = lax.axis_index("student")
    row_count = 1024
    target_raw, sq, student_res, attn_student, ssq = gathered(
        tin, tattn, tw, tgain, proj, sin, sattn, su
    )
    sums = of_everyone(jnp.stack([jnp.sum(sq, axis=1), jnp.sum(ssq, axis=1)]), "teacher")
    teacher_scale = lax.rsqrt(sums[0] / DT + epsilon)
    student_scale = lax.rsqrt(sums[1] / DS + epsilon)
    target_rows = (target_raw.astype(F32) * teacher_scale[:, None]).astype(BF)
    local_rows = lax.dynamic_index_in_dim(
        row_order.reshape(16, 16, 64), s, 1, keepdims=False
    ).reshape(1024) - s * row_count
    pick = (local_rows[:, None] == jnp.arange(1024)[None, :]).astype(BF)
    live_rows = jnp.where(token_ids != PAD_ID, 1.0, 0.0).astype(BF)
    both = jnp.concatenate([target_rows, jnp.broadcast_to(live_rows[:, None], (1024, 128))], axis=1)
    moved = lax.all_to_all(
        jnp.dot(pick, both, preferred_element_type=F32).astype(BF).reshape(16, 64, 640),
        "student", 0, 0, tiled=True,
    ).reshape(1024, 640)
    target = moved[:, :512].astype(F32)
    weight_mask = moved[:, 512].astype(F32)
    normed = student_res * student_scale[:, None]
    gain_values = sgain.astype(F32)[None, :]
    distance = normed * gain_values - target
    loss_weight = 1.0 / math.sqrt(16384)
    grad_out = distance * (weight_mask * loss_weight)[:, None]
    gain_part = jnp.sum(grad_out * normed, axis=0)
    grad_norm = grad_out * gain_values
    inner_sum = of_everyone(jnp.sum(grad_norm * normed, axis=1), "teacher")
    grad_res = (student_scale[:, None] * (grad_norm - normed * (inner_sum / DS)[:, None])).astype(BF)
    parts = lax.dot_general(
        attn_student, grad_res, (((0,), (0,)), ((), ())), preferred_element_type=F32
    ).astype(BF)
    grad_weight = jnp.sum(
        lax.all_to_all(parts.reshape(16, 128, 512), "student", 0, 0, tiled=True).astype(F32), axis=0
    )
    grad_gain = of_everyone(gain_part, "student")
    return (grad_weight, grad_gain)


def solution(mesh):
    placed = (
        P("student", "teacher"),
        P("student", "teacher"),
        P("student", "teacher"),
        P("teacher"),
        P("teacher", "student"),
        P("student", "teacher"),
        P("student", "teacher"),
        P("student", "teacher"),
        P("teacher"),
        P("student"),
        P(),
    )
    return jax.shard_map(
        shards,
        mesh=mesh,
        in_specs=placed,
        out_specs=(P("student", "teacher"), P("teacher")),
        check_vma=False,
    )
```

```python
import math

import jax
import jax.numpy as jnp
from jax import lax
from jax.experimental import pallas as pl
from jax.experimental.pallas import tpu as pltpu
from jax.sharding import PartitionSpec as P

DT = 8192
DS = 4096
PAD_ID = 128004
epsilon = 1e-05

BF = jnp.bfloat16
F32 = jnp.float32
SLOTS = 256
LOSS = 1.0 / math.sqrt(16384)


def div(a, b):
    return lax.div(a, jnp.int32(b))


def rem(a, b):
    return lax.rem(a, jnp.int32(b))


class Place:
    def __init__(self):
        t = lax.axis_index("teacher")
        s = lax.axis_index("student")
        self.t, self.s = t, s
        self.zh, self.y = div(t, 4), rem(t, 4)
        self.zl, self.x, self.core = div(s, 8), rem(div(s, 2), 4), rem(s, 2)
        self.z = self.zh * 2 + self.zl

    def dev(self, dz=0, dy=0, dx=0, dc=0):
        t, s = self.index(dz, dy, dx, dc)
        return {"teacher": t, "student": s}

    def index(self, dz=0, dy=0, dx=0, dc=0):
        z, y, x, c = self.z, self.y, self.x, self.core
        if dz:
            z = rem(z + (dz % 4), 4)
        if dy:
            y = rem(y + (dy % 4), 4)
        if dx:
            x = rem(x + (dx % 4), 4)
        if dc:
            c = 1 - c
        return div(z, 2) * 4 + y, rem(z, 2) * 8 + x * 2 + c


class Net:
    def __init__(self, send, recv):
        self.send, self.recv, self.n, self.open = send, recv, 0, []

    def copy(self, src, dst, device):
        c = pltpu.make_async_remote_copy(
            src_ref=src,
            dst_ref=dst,
            send_sem=self.send.at[self.n],
            recv_sem=self.recv.at[self.n],
            device_id=device,
            device_id_type=pl.DeviceIdType.MESH,
        )
        self.n += 1
        c.start()
        self.open.append(c)
        return c

    def sent(self, copies):
        for c in copies:
            c.wait_send()
        gone = {id(c) for c in copies}
        self.open = [c for c in self.open if id(c) not in gone]

    def finish(self):
        for c in self.open:
            c.wait_send()
        self.open = []


def got(*copies):
    for c in copies:
        c.wait_recv()


def to_rows(lanes, out):
    for q in range(8):
        turned = jnp.transpose(lanes[q * 128 : q * 128 + 128, :])
        out[q : q + 1, :] = jnp.sum(turned, axis=0, keepdims=True)


def to_columns(rows, out):
    for q in range(8):
        wide = jnp.broadcast_to(rows[q : q + 1, :], (128, 128))
        out[q * 128 : q * 128 + 128, :] = jnp.transpose(wide)


def fold(a):
    return a[:, 0:128] + a[:, 128:256] + a[:, 256:384] + a[:, 384:512]


def step_kernel(
    tin, tattn, tw, tgain, proj, sin, sattn, su, sgain, tokens, order,
    weight_out, gain_out,
    bufA, bufC, bufW, bufP, bufU, tinv, sinv, hid,
    tmpA, tmpC, tmpE, r1, r2, r3, zs,
    sq_out, sres_out, ssq_out, target, frecv, gn, sibr, grecv, tok, rowbuf,
    tcol, scol, lcol, stage, exch, gstage, gains,
    send, recv, local,
):
    p = Place()
    up, down = {"dy": 1}, {"dy": -1}
    barrier = pltpu.get_barrier_semaphore()
    teachers = [{"teacher": rem(p.t + j, 8), "student": p.s} for j in range(1, 8)]
    students = [{"teacher": p.t, "student": rem(p.s + j, 16)} for j in range(1, 16)]
    across = {"teacher": rem(p.t + 4, 8), "student": rem(p.s + 8, 16)}
    met = teachers + students + [across]
    for d in met:
        pl.semaphore_signal(barrier, inc=1, device_id=d, device_id_type=pl.DeviceIdType.MESH)
    pl.semaphore_wait(barrier, len(met))
    net = Net(send, recv)

    A = (tattn, bufA, tmpA, 512)
    C = (sattn, bufC, tmpC, 512)
    W = (tw, bufW, 128)
    Q = (proj, bufP, 512)
    U = (su, bufU, 64)

    def own(arr, h):
        half = arr[-1]
        return arr[0].at[pl.ds(h * half, half), :]

    def slot(arr, i, h):
        half = arr[-1]
        return arr[1].at[i, pl.ds(h * half, half), :]

    tp = p.index(dz=2)[0]
    zpart = {"teacher": p.t, "student": rem(p.s + 8, 16)}
    sp = rem(p.s + 8, 16)
    sib = p.dev(dc=1)
    sib_index = p.index(dc=1)[1]
    locals_ = []

    def bring(src, dst):
        c = pltpu.make_async_copy(src, dst, local.at[len(locals_)])
        c.start()
        locals_.append(c)
        return c

    def t_own(arr):
        ups = [net.copy(own(arr, h), slot(arr, p.t, h), p.dev(dy=1)) for h in (0, 1)]
        downs = [net.copy(own(arr, h), slot(arr, p.t, h), p.dev(dy=-1)) for h in (1, 0)][::-1]
        return ups, downs

    def t_hop1(arr):
        return [
            net.copy(own(arr, 0), arr[2].at[0], p.dev(dz=1)),
            net.copy(own(arr, 1), arr[2].at[1], p.dev(dz=-1)),
        ]

    def t_hop2(arr, hop1):
        got(hop1[0])
        a = net.copy(arr[2].at[0], slot(arr, p.index(dz=-1)[0], 0), p.dev(dz=1))
        got(hop1[1])
        b = net.copy(arr[2].at[1], slot(arr, p.index(dz=1)[0], 1), p.dev(dz=-1))
        return [a, b]

    def t_forward(arr, ups, downs, dz):
        got(ups[0])
        a = net.copy(slot(arr, p.index(dz=dz, dy=-1)[0], 0), slot(arr, p.index(dz=dz, dy=-1)[0], 0), p.dev(dy=1))
        got(downs[1])
        b = net.copy(slot(arr, p.index(dz=dz, dy=1)[0], 1), slot(arr, p.index(dz=dz, dy=1)[0], 1), p.dev(dy=-1))
        return [a, b]

    def t_partner(arr, hop2):
        got(*hop2)
        ups = [net.copy(slot(arr, tp, h), slot(arr, tp, h), p.dev(dy=1)) for h in (0, 1)]
        downs = [net.copy(slot(arr, tp, h), slot(arr, tp, h), p.dev(dy=-1)) for h in (1, 0)][::-1]
        return ups, downs

    def s_own(arr):
        ups = [net.copy(own(arr, h), slot(arr, p.s, h), p.dev(dx=1)) for h in (0, 1)]
        downs = [net.copy(own(arr, h), slot(arr, p.s, h), p.dev(dx=-1)) for h in (1, 0)][::-1]
        return ups, downs

    def s_side(arr):
        return net.copy(arr[0], arr[1].at[p.s], zpart)

    def s_partner(arr, side):
        got(side)
        ups = [net.copy(slot(arr, sp, h), slot(arr, sp, h), p.dev(dx=1)) for h in (0, 1)]
        downs = [net.copy(slot(arr, sp, h), slot(arr, sp, h), p.dev(dx=-1)) for h in (1, 0)][::-1]
        return ups, downs

    def s_index(dx, other):
        i = p.index(dx=dx)[1]
        return rem(i + 8, 16) if other else i

    def s_forward(arr, ups, downs, other):
        got(ups[0])
        i = s_index(-1, other)
        a = net.copy(slot(arr, i, 0), slot(arr, i, 0), p.dev(dx=1))
        got(downs[1])
        j = s_index(1, other)
        b = net.copy(slot(arr, j, 1), slot(arr, j, 1), p.dev(dx=-1))
        return [a, b]

    def share(arr, i):
        return net.copy(arr[1].at[i], arr[1].at[i], sib)

    ssides, sowns, shared = {}, {}, []
    aown = t_own(A)
    ahop1 = t_hop1(A)
    for n, arr in (("W", W), ("Q", Q)):
        sowns[n] = s_own(arr)
        ssides[n] = s_side(arr)
        shared.append(net.copy(arr[0], arr[1].at[p.s], sib))
    bring(tattn, bufA.at[p.t])
    bring(tw, bufW.at[p.s])
    bring(proj, bufP.at[p.s])
    bring(tin, tinv)
    bring(sattn, bufC.at[p.t])
    bring(su, bufU.at[p.s])
    bring(sin, sinv)
    cown = t_own(C)
    told = [net.copy(tokens, tok.at[p.s], d) for d in students]
    bring(tokens, tok.at[p.s])

    ahop2 = t_hop2(A, ahop1)
    chop1 = t_hop1(C)
    sowns["U"] = s_own(U)
    ssides["U"] = s_side(U)
    shared.append(net.copy(U[0], U[1].at[p.s], sib))
    S = (("W", W), ("Q", Q), ("U", U))
    sfwd, sfwd2, sparts = {}, {}, {}
    for n, arr in S[:2]:
        sfwd[n] = s_forward(arr, *sowns[n], False)
    afwd = t_forward(A, *aown, 0)
    for n, arr in S[:2]:
        sparts[n] = s_partner(arr, ssides[n])
    apart = t_partner(A, ahop2)
    chop2 = t_hop2(C, chop1)
    for n, arr in S[:2]:
        got(sowns[n][0][1], sowns[n][1][0])
        shared.append(share(arr, sp))
        shared.append(share(arr, s_index(-1, False)))
        shared.append(share(arr, s_index(1, False)))
    sfwd["U"] = s_forward(U, *sowns["U"], False)
    sparts["U"] = s_partner(U, ssides["U"])
    for n, arr in S[:2]:
        sfwd2[n] = s_forward(arr, *sparts[n], True)
    afwd2 = t_forward(A, *apart, 2)
    cfwd = t_forward(C, *cown, 0)
    cpart = t_partner(C, chop2)
    for n, arr in S[:2]:
        got(*sfwd[n], sparts[n][0][1], sparts[n][1][0])
        shared.append(share(arr, s_index(2, False)))
        shared.append(share(arr, s_index(-1, True)))
        shared.append(share(arr, s_index(1, True)))
    sfwd2["U"] = s_forward(U, *sparts["U"], True)
    for n, arr in S[:2]:
        got(*sfwd2[n])
        shared.append(share(arr, s_index(2, True)))
    got(sowns["U"][0][1], sowns["U"][1][0], sparts["U"][0][1], sparts["U"][1][0], *sfwd["U"])
    ushared = [
        share(U, sp),
        share(U, s_index(-1, False)),
        share(U, s_index(1, False)),
        share(U, s_index(2, False)),
        share(U, s_index(-1, True)),
        share(U, s_index(1, True)),
    ]
    got(aown[0][1], aown[1][0], *afwd, apart[0][1], apart[1][0], *afwd2)
    got(*shared)
    for c in locals_:
        c.wait()

    sq_out[...] = jnp.zeros_like(sq_out)

    def first(i, carry):
        rows = pl.ds(pl.multiple_of(div(i, 2) * 512, 512), 512)
        cols = pl.ds(pl.multiple_of(rem(i, 2) * 512, 512), 512)
        acc = tinv[rows, cols].astype(F32)
        for t in range(8):
            w = bufW[2 * t : 2 * t + 2, :, cols].reshape(512, 512)
            acc = acc + jnp.dot(bufA[t, rows, :], w, preferred_element_type=F32)
        square = acc * acc
        sq_out[rows, :] += square[:, 0:128] + square[:, 128:256] + square[:, 256:384] + square[:, 384:512]
        hid[rows, cols] = (acc * tgain[:, cols]).astype(BF)
        return carry

    lax.fori_loop(0, 2, first, 0)
    cfwd2 = t_forward(C, *cpart, 2)
    lax.fori_loop(2, 4, first, 0)
    early = list(net.open)
    a_sends = [*aown[0], *aown[1], *ahop1, *ahop2, *afwd, *apart[0], *apart[1], *afwd2]
    net.sent(a_sends)
    gone = {id(c) for c in a_sends}
    early = [c for c in early if id(c) not in gone]

    def project(k):
        def step(i, carry):
            rows = pl.ds(pl.multiple_of(i * 512, 512), 512)
            h = hid[rows, :]
            bufA[k, rows, 0:256] = jnp.dot(h, bufP[2 * k], preferred_element_type=F32).astype(BF)
            bufA[k, rows, 256:512] = jnp.dot(h, bufP[2 * k + 1], preferred_element_type=F32).astype(BF)
            return carry

        lax.fori_loop(0, 2, step, 0)

    def block(far, dy):
        zh = 1 - p.zh if far else p.zh
        y = rem(p.y + (dy % 4), 4)
        return zh * 4 + y

    lo, hi = pl.ds(0, 512), pl.ds(512, 512)

    def opening(n, far):
        k = block(far, 2)
        project(k)
        return (
            net.copy(bufA.at[k, lo, :], r1.at[n, 0], p.dev(dy=1)),
            net.copy(bufA.at[k, hi, :], r1.at[n, 1], p.dev(dy=-1)),
        )

    def plain(n, far):
        ku, kd = block(far, 1), block(far, -1)
        project(ku)
        u = net.copy(bufA.at[ku, hi, :], r2.at[n, 0, hi, :], p.dev(dy=1))
        project(kd)
        d = net.copy(bufA.at[kd, lo, :], r2.at[n, 1, lo, :], p.dev(dy=-1))
        return u, d

    def added(n, far, opened):
        ku, kd = block(far, 1), block(far, -1)

        def add(k, base, j):
            def step(i, carry):
                at = pl.ds(pl.multiple_of(i * 128, 128), 128)
                rows = pl.ds(pl.multiple_of(base + i * 128, 128), 128)
                bufA[k, rows, :] = (bufA[k, rows, :].astype(F32) + r1[n, j, at, :].astype(F32)).astype(BF)
                return carry

            lax.fori_loop(0, 4, step, 0)

        got(opened[0])
        add(ku, 0, 0)
        u = net.copy(bufA.at[ku, lo, :], r2.at[n, 0, lo, :], p.dev(dy=1))
        got(opened[1])
        add(kd, 512, 1)
        d = net.copy(bufA.at[kd, hi, :], r2.at[n, 1, hi, :], p.dev(dy=-1))
        return u, d

    open_far = opening(0, True)
    plain_far = plain(0, True)
    open_near = opening(1, False)
    added_far = added(0, True, open_far)
    plain_near = plain(1, False)
    added_near = added(1, False, open_near)
    k_far, k_near = block(True, 0), block(False, 0)
    project(k_far)
    project(k_near)

    def exchange(kind):
        return [net.copy(stage.at[kind], exch.at[kind, p.t], d) for d in teachers]

    def exchanged(kind, copies):
        exch[kind, p.t] = stage[kind]
        got(*copies)
        total = exch[kind, 0]
        for t in range(1, 8):
            total = total + exch[kind, t]
        return total

    to_rows(sq_out, stage.at[0])
    tsums = exchange(0)

    got(cown[0][1], cown[1][0], *cfwd, cpart[0][1], cpart[1][0], *cfwd2)
    got(*sfwd2["U"])
    ushared.append(share(U, s_index(2, True)))
    got(*ushared)

    def student(i, carry):
        rows = pl.ds(pl.multiple_of(i * 512, 512), 512)
        acc = sinv[rows, :].astype(F32)
        for t in range(8):
            w = bufU[2 * t : 2 * t + 2].reshape(256, 512)
            acc = acc + jnp.dot(bufC[t, rows, :], w, preferred_element_type=F32)
        ssq_out[rows, :] = fold(acc * acc)
        sres_out[rows, :] = acc
        return carry

    lax.fori_loop(0, 2, student, 0)
    to_rows(ssq_out, stage.at[1])
    ssums = exchange(1)

    net.sent(early)

    def turn(i, carry):
        t = div(i, 8)
        rows = pl.ds(pl.multiple_of(rem(i, 8) * 128, 128), 128)
        block = bufC[t, rows, :].astype(F32)
        at = pl.ds(pl.multiple_of(rem(t, 2) * 128, 128), 128)
        for core in range(2):
            turned = jnp.transpose(block[:, core * 128 : core * 128 + 128])
            bufW[core * 4 + div(t, 2), at, rows] = turned.astype(BF)
        return carry

    lax.fori_loop(0, 64, turn, 0)

    wide = lax.broadcasted_iota(jnp.int32, (64, 1024), 1).astype(F32)
    narrow = lax.broadcasted_iota(jnp.int32, (64, 128), 1).astype(F32)
    rowbuf[...] = jnp.zeros_like(rowbuf)
    for m in range(16):
        b = rem(p.s + m, 16)
        rowbuf[0, m : m + 1, :] = order[pl.ds(b * 8 + div(p.s, 2), 1), :].astype(F32)
    rowbuf[1, 0:8, :] = order[pl.ds(pl.multiple_of(p.s * 8, 8), 8), :].astype(F32)
    for n in range(2):
        rowbuf[2 + n] = jnp.transpose(rowbuf[n])
    half = pl.ds(pl.multiple_of(rem(p.s, 2) * 64, 64), 64)
    base = (p.s * 1024).astype(F32)
    mine = rowbuf[2, half, :] - base
    for m in range(16):
        hid[m * 64 : m * 64 + 64, :] = jnp.where(wide == mine[:, m : m + 1], 1.0, 0.0).astype(BF)

    got(*told)
    for b in range(16):
        low = (b % 2) * 64
        named = rowbuf[3, low : low + 64, b // 2 : b // 2 + 1] - float(b * 1024)
        live = jnp.where(tok[b] != PAD_ID, LOSS, 0.0)
        acc = jnp.zeros((64, 128), F32)
        for q in range(8):
            acc = acc + jnp.where(narrow == named - float(q * 128), live[q : q + 1, :], 0.0)
        total = jnp.sum(acc, axis=1, keepdims=True)
        lcol[b * 64 : b * 64 + 64, :] = jnp.broadcast_to(total, (64, 128))

    to_columns(lax.rsqrt(exchanged(0, tsums) / DT + epsilon), tcol)
    to_columns(lax.rsqrt(exchanged(1, ssums) / DS + epsilon), scol)

    def three(n, k, base, i):
        at = pl.ds(pl.multiple_of(base + i * 128, 128), 128)
        return at, (
            bufA[k, at, :].astype(F32) + r2[n, 0, at, :].astype(F32) + r2[n, 1, at, :].astype(F32)
        )

    got(*plain_far, *added_far)

    def far_sum(i, carry):
        at, total = three(0, k_far, 0, i)
        zs[at, :] = total.astype(BF)
        return carry

    lax.fori_loop(0, 8, far_sum, 0)
    hop1 = (
        net.copy(zs.at[lo, :], tmpE.at[0], p.dev(dz=1)),
        net.copy(zs.at[hi, :], tmpE.at[1], p.dev(dz=-1)),
    )
    got(hop1[0])
    h2a = net.copy(tmpE.at[0], r3.at[lo, :], p.dev(dz=1))
    got(hop1[1])
    h2b = net.copy(tmpE.at[1], r3.at[hi, :], p.dev(dz=-1))
    got(*plain_near, *added_near)
    got(h2a, h2b)

    def near_sum(i, carry):
        at, total = three(1, k_near, 0, i)
        total = total + r3[at, :].astype(F32)
        target[at, :] = (total * tcol[at, 0:1]).astype(BF)
        return carry

    lax.fori_loop(0, 8, near_sum, 0)

    moved = {}
    left, right = pl.ds(0, 512), pl.ds(512, 512)
    for group in (1, 2, 3, 0):
        picked = jnp.dot(
            hid[group * 256 : group * 256 + 256, :], target[...], preferred_element_type=F32
        ).astype(BF)
        tinv[group * 256 : group * 256 + 256, 0:512] = picked
        if group == 0:
            frecv[p.s] = picked[0:64, :]
        for m in range(max(group * 4, 1), group * 4 + 4):
            moved[m] = net.copy(tinv.at[m * 64 : m * 64 + 64, left], frecv.at[p.s], students[m - 1])

    gain_values = sgain[...]
    partial = jnp.zeros((1, 512), F32)
    for m in (0, *range(4, 16), 1, 2, 3):
        if m:
            got(moved[m])
        b = rem(p.s + (16 - m), 16)
        rows = pl.ds(pl.multiple_of(b * 64, 64), 64)
        normed = sres_out[rows, :] * scol[rows, 0:1]
        grad_out = (normed * gain_values - frecv[b].astype(F32)) * lcol[rows, 0:1]
        partial = partial + jnp.sum(grad_out * normed, axis=0, keepdims=True)
        grad_norm = grad_out * gain_values
        gn[rows, :] = grad_norm
        ssq_out[rows, :] = fold(grad_norm * normed)
    to_rows(ssq_out, stage.at[2])
    inner = exchange(2)
    gstage[...] = partial
    gained = [net.copy(gstage, gains.at[p.s], d) for d in students]
    net.sent(hop1)
    to_columns(exchanged(2, inner) / DS, sq_out)

    def grad(i, carry):
        rows = pl.ds(pl.multiple_of(i * 128, 128), 128)
        scale = scol[rows, 0:1]
        normed = sres_out[rows, :] * scale
        zs[rows, :] = (scale * (gn[rows, :] - normed * sq_out[rows, 0:1])).astype(BF)
        return carry

    lax.fori_loop(0, 8, grad, 0)

    def product(core, i):
        return jnp.dot(bufW[core * 4 + i], zs[...], preferred_element_type=F32)

    halves = []
    for i in range(4):
        sinv[i * 256 : i * 256 + 256, :] = product(1 - p.core, i).astype(BF)
        part = pl.ds(i * 256, 256)
        halves.append(net.copy(sinv.at[part, :], sibr.at[part, :], sib))
    for i in range(4):
        own_part = product(p.core, i)
        got(halves[i])
        total = own_part + sibr[i * 256 : i * 256 + 256, :].astype(F32)
        tinv[i * 256 : i * 256 + 256, 512:1024] = total.astype(BF)
    chip = div(p.s, 2)
    parts = []
    for m in range(1, 8):
        q = rem(chip + m, 8)
        rows = pl.ds(pl.multiple_of(q * 128, 128), 128)
        to = {"teacher": p.t, "student": q * 2 + p.core}
        parts.append(net.copy(tinv.at[rows, right], grecv.at[m - 1], to))
    gains[p.s] = gstage[...]
    got(*gained)
    total_gain = gains[0]
    for b in range(1, 16):
        total_gain = total_gain + gains[b]
    gain_out[...] = total_gain
    total = tinv[pl.ds(pl.multiple_of(chip * 128, 128), 128), 512:1024].astype(F32)
    for m in range(7):
        got(parts[m])
        total = total + grecv[m].astype(F32)
    weight_out[...] = total
    net.finish()


def step(tin, tattn, tw, tgain, proj, sin, sattn, su, sgain, token_ids, row_order):
    anywhere = pl.BlockSpec(memory_space=pl.ANY)
    vmem = pl.BlockSpec(memory_space=pltpu.VMEM)
    V = pltpu.VMEM
    weight, gain = pl.pallas_call(
        step_kernel,
        out_shape=(
            jax.ShapeDtypeStruct((128, 512), F32),
            jax.ShapeDtypeStruct((1, 512), F32),
        ),
        in_specs=[anywhere] * 3 + [vmem] + [anywhere] * 4 + [vmem, anywhere, vmem],
        out_specs=(vmem, vmem),
        scratch_shapes=[
            V((8, 1024, 512), BF),
            V((8, 1024, 256), BF),
            V((16, 256, 1024), BF),
            V((16, 1024, 256), BF),
            V((16, 128, 512), BF),
            V((1024, 1024), BF),
            V((1024, 512), BF),
            V((1024, 1024), BF),
            V((2, 512, 512), BF),
            V((2, 512, 256), BF),
            V((2, 512, 512), BF),
            V((2, 2, 512, 512), BF),
            V((2, 2, 1024, 512), BF),
            V((1024, 512), BF),
            V((1024, 512), BF),
            V((1024, 128), F32),
            V((1024, 512), F32),
            V((1024, 128), F32),
            V((1024, 512), BF),
            V((16, 64, 512), BF),
            V((1024, 512), F32),
            V((1024, 512), BF),
            V((7, 128, 512), BF),
            V((16, 8, 128), jnp.int32),
            V((4, 128, 128), F32),
            V((1024, 128), F32),
            V((1024, 128), F32),
            V((1024, 128), F32),
            V((3, 8, 128), F32),
            V((3, 8, 8, 128), F32),
            V((1, 512), F32),
            V((16, 1, 512), F32),
            pltpu.SemaphoreType.DMA((SLOTS,)),
            pltpu.SemaphoreType.DMA((SLOTS,)),
            pltpu.SemaphoreType.DMA((16,)),
        ],
        compiler_params=pltpu.CompilerParams(
            collective_id=0, has_side_effects=True, vmem_limit_bytes=67043328
        ),
        name="step",
    )(
        tin, tattn, tw, tgain.astype(F32).reshape(1, -1), proj, sin, sattn, su,
        sgain.astype(F32).reshape(1, -1), token_ids.reshape(8, 128), row_order.reshape(128, 128),
    )
    return weight, gain.reshape(512)


def solution(mesh):
    placed = (
        P("student", "teacher"),
        P("student", "teacher"),
        P("student", "teacher"),
        P("teacher"),
        P("teacher", "student"),
        P("student", "teacher"),
        P("student", "teacher"),
        P("student", "teacher"),
        P("teacher"),
        P("student"),
        P(),
    )
    return jax.shard_map(
        step,
        mesh=mesh,
        in_specs=placed,
        out_specs=(P("student", "teacher"), P("teacher")),
        check_vma=False,
    )
```

```python
import math

import jax
import jax.numpy as jnp
from jax import lax
from jax.experimental import pallas as pl
from jax.experimental.pallas import tpu as pltpu
from jax.sharding import PartitionSpec as P

DT = 8192
DS = 4096
PAD_ID = 128004
epsilon = 1e-05

BF = jnp.bfloat16
F32 = jnp.float32
SLOTS = 256
LOSS = 1.0 / math.sqrt(16384)


def div(a, b):
    return lax.div(a, jnp.int32(b))


def rem(a, b):
    return lax.rem(a, jnp.int32(b))


class Place:
    def __init__(self):
        t = lax.axis_index("teacher")
        s = lax.axis_index("student")
        self.t, self.s = t, s
        self.zh, self.y = div(t, 4), rem(t, 4)
        self.zl, self.x, self.core = div(s, 8), rem(div(s, 2), 4), rem(s, 2)
        self.z = self.zh * 2 + self.zl

    def dev(self, dz=0, dy=0, dx=0, dc=0):
        t, s = self.index(dz, dy, dx, dc)
        return {"teacher": t, "student": s}

    def index(self, dz=0, dy=0, dx=0, dc=0):
        z, y, x, c = self.z, self.y, self.x, self.core
        if dz:
            z = rem(z + (dz % 4), 4)
        if dy:
            y = rem(y + (dy % 4), 4)
        if dx:
            x = rem(x + (dx % 4), 4)
        if dc:
            c = 1 - c
        return div(z, 2) * 4 + y, rem(z, 2) * 8 + x * 2 + c


class Net:
    def __init__(self, send, recv):
        self.send, self.recv, self.n, self.open = send, recv, 0, []

    def copy(self, src, dst, device):
        c = pltpu.make_async_remote_copy(
            src_ref=src,
            dst_ref=dst,
            send_sem=self.send.at[self.n],
            recv_sem=self.recv.at[self.n],
            device_id=device,
            device_id_type=pl.DeviceIdType.MESH,
        )
        self.n += 1
        c.start()
        self.open.append(c)
        return c

    def sent(self, copies):
        for c in copies:
            c.wait_send()
        gone = {id(c) for c in copies}
        self.open = [c for c in self.open if id(c) not in gone]

    def finish(self):
        for c in self.open:
            c.wait_send()
        self.open = []


def got(*copies):
    for c in copies:
        c.wait_recv()


def to_rows(lanes, out):
    for q in range(8):
        turned = jnp.transpose(lanes[q * 128 : q * 128 + 128, :])
        out[q : q + 1, :] = jnp.sum(turned, axis=0, keepdims=True)


def to_columns(rows, out):
    for q in range(8):
        wide = jnp.broadcast_to(rows[q : q + 1, :], (128, 128))
        out[q * 128 : q * 128 + 128, :] = jnp.transpose(wide)


def fold(a):
    return a[:, 0:128] + a[:, 128:256] + a[:, 256:384] + a[:, 384:512]


def step_kernel(
    tin, tattn, tw, tgain, proj, sin, sattn, su, sgain, tokens, order,
    weight_out, gain_out,
    bufA, bufC, bufW, bufP, bufU, tinv, sinv, hid,
    pick, tmpA, tmpC, tmpD, tmpE, tmpZ, rz, r1, r2, b1, b2, r3, zs,
    sq_out, sres_out, ssq_out, target, frecv, gn, sibr, grecv, tok, rowbuf,
    scol, lcol, stage, exch, gstage, gains,
    send, recv, local,
):
    p = Place()
    up, down = {"dy": 1}, {"dy": -1}
    barrier = pltpu.get_barrier_semaphore()
    teachers = [{"teacher": rem(p.t + j, 8), "student": p.s} for j in range(1, 8)]
    students = [{"teacher": p.t, "student": rem(p.s + j, 16)} for j in range(1, 16)]
    across = {"teacher": rem(p.t + 4, 8), "student": rem(p.s + 8, 16)}
    met = teachers + students + [across]
    for d in met:
        pl.semaphore_signal(barrier, inc=1, device_id=d, device_id_type=pl.DeviceIdType.MESH)
    pl.semaphore_wait(barrier, len(met))
    net = Net(send, recv)

    A = (tattn, bufA, tmpA, pl.ds(0, 512), 512)
    C = (sattn, bufC, tmpC, pl.ds(0, 128), 512)
    D = (sattn, bufC, tmpD, pl.ds(128, 128), 512)
    W = (tw, bufW, None, pl.ds(0, 1024), 128)
    Q = (proj, bufP, None, pl.ds(0, 256), 512)
    U = (su, bufU, None, pl.ds(0, 512), 64)

    def own(arr, h):
        half = arr[-1]
        return arr[0].at[pl.ds(h * half, half), arr[3]]

    def slot(arr, i, h):
        half = arr[-1]
        return arr[1].at[i, pl.ds(h * half, half), arr[3]]

    tp = p.index(dz=2)[0]
    zpart = {"teacher": p.t, "student": rem(p.s + 8, 16)}
    sp = rem(p.s + 8, 16)
    sib = p.dev(dc=1)
    sib_index = p.index(dc=1)[1]
    locals_ = []

    def bring(src, dst):
        c = pltpu.make_async_copy(src, dst, local.at[len(locals_)])
        c.start()
        locals_.append(c)
        return c

    def t_own(arr):
        ups = [net.copy(own(arr, h), slot(arr, p.t, h), p.dev(dy=1)) for h in (0, 1)]
        downs = [net.copy(own(arr, h), slot(arr, p.t, h), p.dev(dy=-1)) for h in (1, 0)][::-1]
        return ups, downs

    def t_hop1(arr):
        return [
            net.copy(own(arr, 0), arr[2].at[0], p.dev(dz=1)),
            net.copy(own(arr, 1), arr[2].at[1], p.dev(dz=-1)),
        ]

    def t_hop2(arr, hop1):
        got(hop1[0])
        a = net.copy(arr[2].at[0], slot(arr, p.index(dz=-1)[0], 0), p.dev(dz=1))
        got(hop1[1])
        b = net.copy(arr[2].at[1], slot(arr, p.index(dz=1)[0], 1), p.dev(dz=-1))
        return [a, b]

    def t_forward(arr, ups, downs, dz):
        got(ups[0])
        a = net.copy(slot(arr, p.index(dz=dz, dy=-1)[0], 0), slot(arr, p.index(dz=dz, dy=-1)[0], 0), p.dev(dy=1))
        got(downs[1])
        b = net.copy(slot(arr, p.index(dz=dz, dy=1)[0], 1), slot(arr, p.index(dz=dz, dy=1)[0], 1), p.dev(dy=-1))
        return [a, b]

    def t_partner(arr, hop2):
        got(*hop2)
        ups = [net.copy(slot(arr, tp, h), slot(arr, tp, h), p.dev(dy=1)) for h in (0, 1)]
        downs = [net.copy(slot(arr, tp, h), slot(arr, tp, h), p.dev(dy=-1)) for h in (1, 0)][::-1]
        return ups, downs

    def d_hop1(dy, halves=(0, 1)):
        out = []
        for h in halves:
            src = own(D, h) if dy == 0 else slot(D, p.index(dy=dy)[0], h)
            out.append(net.copy(src, tmpD.at[dy % 4, h], p.dev(dz=(1, -1)[h])))
        return out

    def d_hop2(dy, hop1):
        out = []
        for h, c in enumerate(hop1):
            got(c)
            at = slot(D, p.index(dz=(-1, 1)[h], dy=dy)[0], h)
            out.append(net.copy(tmpD.at[dy % 4, h], at, p.dev(dz=(1, -1)[h])))
        return out

    def s_own(arr):
        ups = [net.copy(own(arr, h), slot(arr, p.s, h), p.dev(dx=1)) for h in (0, 1)]
        downs = [net.copy(own(arr, h), slot(arr, p.s, h), p.dev(dx=-1)) for h in (1, 0)][::-1]
        return ups, downs

    def s_side(arr):
        return net.copy(arr[0], arr[1].at[p.s], zpart)

    def s_partner(arr, side):
        got(side)
        ups = [net.copy(slot(arr, sp, h), slot(arr, sp, h), p.dev(dx=1)) for h in (0, 1)]
        downs = [net.copy(slot(arr, sp, h), slot(arr, sp, h), p.dev(dx=-1)) for h in (1, 0)][::-1]
        return ups, downs

    def s_index(dx, other):
        i = p.index(dx=dx)[1]
        return rem(i + 8, 16) if other else i

    def s_forward(arr, ups, downs, other):
        got(ups[0])
        i = s_index(-1, other)
        a = net.copy(slot(arr, i, 0), slot(arr, i, 0), p.dev(dx=1))
        got(downs[1])
        j = s_index(1, other)
        b = net.copy(slot(arr, j, 1), slot(arr, j, 1), p.dev(dx=-1))
        return [a, b]

    def share(arr, i):
        return net.copy(arr[1].at[i], arr[1].at[i], sib)

    ssides, sowns, shared = {}, {}, []
    aown = t_own(A)
    ahop1 = t_hop1(A)
    for n, arr in (("W", W), ("Q", Q)):
        sowns[n] = s_own(arr)
        ssides[n] = s_side(arr)
        shared.append(net.copy(arr[0], arr[1].at[p.s], sib))
    bring(tattn, bufA.at[p.t])
    bring(tw, bufW.at[p.s])
    bring(proj, bufP.at[p.s])
    bring(tin, tinv)
    bring(sattn, bufC.at[p.t])
    bring(su, bufU.at[p.s])
    bring(sin, sinv)
    down_ = t_own(D)
    told = [net.copy(tokens, tok.at[p.s], d) for d in students]
    bring(tokens, tok.at[p.s])
    sowns["U"] = s_own(U)
    ssides["U"] = s_side(U)
    shared.append(net.copy(U[0], U[1].at[p.s], sib))
    S = (("W", W), ("Q", Q), ("U", U))
    sfwd, sfwd2, sparts = {}, {}, {}

    ahop2 = t_hop2(A, ahop1)
    dhop1, dhop2 = {}, {}
    dhop1[0] = d_hop1(0)
    for n, arr in S[:2]:
        sfwd[n] = s_forward(arr, *sowns[n], False)
    afwd = t_forward(A, *aown, 0)
    sparts["W"] = s_partner(W, ssides["W"])
    dhop2[0] = d_hop2(0, dhop1[0])
    sparts["Q"] = s_partner(Q, ssides["Q"])
    apart = t_partner(A, ahop2)
    dfwd = t_forward(D, *down_, 0)
    got(down_[0][1], down_[1][0])
    dhop1[-1] = d_hop1(-1)
    dhop1[1] = d_hop1(1)
    for n, arr in S[:2]:
        got(sowns[n][0][1], sowns[n][1][0])
        shared.append(share(arr, sp))
        shared.append(share(arr, s_index(-1, False)))
        shared.append(share(arr, s_index(1, False)))
    sfwd["U"] = s_forward(U, *sowns["U"], False)
    sparts["U"] = s_partner(U, ssides["U"])
    dhop2[-1] = d_hop2(-1, dhop1[-1])
    dhop2[1] = d_hop2(1, dhop1[1])
    for n, arr in S[:2]:
        sfwd2[n] = s_forward(arr, *sparts[n], True)
    afwd2 = t_forward(A, *apart, 2)
    chop1 = t_hop1(C)
    got(*dfwd)
    dhop1[2] = d_hop1(2)
    cown = t_own(C)
    chop2 = t_hop2(C, chop1)
    dhop2[2] = d_hop2(2, dhop1[2])
    for n, arr in S[:2]:
        got(*sfwd[n], sparts[n][0][1], sparts[n][1][0])
        shared.append(share(arr, s_index(2, False)))
        shared.append(share(arr, s_index(-1, True)))
        shared.append(share(arr, s_index(1, True)))
    sfwd2["U"] = s_forward(U, *sparts["U"], True)
    got(sowns["U"][0][1], sowns["U"][1][0], sparts["U"][0][1], sparts["U"][1][0], *sfwd["U"])
    ushared = [
        share(U, sp),
        share(U, s_index(-1, False)),
        share(U, s_index(1, False)),
        share(U, s_index(2, False)),
        share(U, s_index(-1, True)),
        share(U, s_index(1, True)),
    ]
    for c in locals_:
        c.wait()

    wide = lax.broadcasted_iota(jnp.int32, (64, 1024), 1).astype(F32)
    narrow = lax.broadcasted_iota(jnp.int32, (64, 128), 1).astype(F32)
    rowbuf[...] = jnp.zeros_like(rowbuf)
    for m in range(16):
        b = rem(p.s + m, 16)
        rowbuf[0, m : m + 1, :] = order[pl.ds(b * 8 + div(p.s, 2), 1), :].astype(F32)
    rowbuf[1, 0:8, :] = order[pl.ds(pl.multiple_of(p.s * 8, 8), 8), :].astype(F32)
    for n in range(2):
        rowbuf[2 + n] = jnp.transpose(rowbuf[n])
    half = pl.ds(pl.multiple_of(rem(p.s, 2) * 64, 64), 64)
    base = (p.s * 1024).astype(F32)
    mine = rowbuf[2, half, :] - base
    for m in range(16):
        pick[m * 64 : m * 64 + 64, :] = jnp.where(wide == mine[:, m : m + 1], 1.0, 0.0).astype(BF)

    got(*told)
    for b in range(16):
        low = (b % 2) * 64
        named = rowbuf[3, low : low + 64, b // 2 : b // 2 + 1] - float(b * 1024)
        live = jnp.where(tok[b] != PAD_ID, LOSS, 0.0)
        acc = jnp.zeros((64, 128), F32)
        for q in range(8):
            acc = acc + jnp.where(narrow == named - float(q * 128), live[q : q + 1, :], 0.0)
        total = jnp.sum(acc, axis=1, keepdims=True)
        lcol[b * 64 : b * 64 + 64, :] = jnp.broadcast_to(total, (64, 128))

    for n, arr in S[:2]:
        got(*sfwd2[n])
        shared.append(share(arr, s_index(2, True)))
    got(aown[0][1], aown[1][0], *afwd, apart[0][1], apart[1][0], *afwd2)
    cfwd = t_forward(C, *cown, 0)
    cpart = t_partner(C, chop2)
    got(*shared)
    sq_out[...] = jnp.zeros_like(sq_out)

    def first(i, carry):
        rows = pl.ds(pl.multiple_of(div(i, 2) * 512, 512), 512)
        cols = pl.ds(pl.multiple_of(rem(i, 2) * 512, 512), 512)
        acc = tinv[rows, cols].astype(F32)
        for t in range(8):
            w = bufW[2 * t : 2 * t + 2, :, cols].reshape(512, 512)
            acc = acc + jnp.dot(bufA[t, rows, :], w, preferred_element_type=F32)
        square = acc * acc
        sq_out[rows, :] += square[:, 0:128] + square[:, 128:256] + square[:, 256:384] + square[:, 384:512]
        hid[rows, cols] = (acc * tgain[:, cols]).astype(BF)
        return carry

    lax.fori_loop(0, 2, first, 0)
    cfwd2 = t_forward(C, *cpart, 2)
    lax.fori_loop(2, 4, first, 0)
    early = list(net.open)
    a_sends = [*aown[0], *aown[1], *ahop1, *ahop2, *afwd, *apart[0], *apart[1], *afwd2]
    net.sent(a_sends)
    gone = {id(c) for c in a_sends}
    early = [c for c in early if id(c) not in gone]

    def columns(half):
        return pl.ds(half * 256, 256)

    def project(k, half):
        def step(i, carry):
            rows = pl.ds(pl.multiple_of(i * 512, 512), 512)
            bufA[k, rows, columns(half)] = jnp.dot(
                hid[rows, :], bufP[2 * k + half], preferred_element_type=F32
            ).astype(BF)
            return carry

        lax.fori_loop(0, 2, step, 0)

    def block(far, dy):
        zh = 1 - p.zh if far else p.zh
        y = rem(p.y + (dy % 4), 4)
        return zh * 4 + y

    lo, hi = pl.ds(0, 512), pl.ds(512, 512)
    right = pl.ds(512, 512)

    def add(k, half, base, count, ref, rebase):
        def step(i, carry):
            at = pl.ds(pl.multiple_of(rebase + i * 128, 128), 128)
            rows = pl.ds(pl.multiple_of(base + i * 128, 128), 128)
            both = bufA[k, rows, columns(half)].astype(F32) + ref[at, :].astype(F32)
            bufA[k, rows, columns(half)] = both.astype(BF)
            return carry

        lax.fori_loop(0, count, step, 0)

    def piece(k, half, rows):
        return bufA.at[k, rows, columns(half)]

    def open_to(k, half, dst):
        return (
            net.copy(piece(k, half, lo), dst.at[0], p.dev(dy=1)),
            net.copy(piece(k, half, hi), dst.at[1], p.dev(dy=-1)),
        )

    def added(far, half, opened, src, dst):
        ku, kd = block(far, 1), block(far, -1)
        got(opened[0])
        add(ku, half, 0, 4, src.at[0], 0)
        u = net.copy(piece(ku, half, lo), dst.at[0, lo, :], p.dev(dy=1))
        got(opened[1])
        add(kd, half, 512, 4, src.at[1], 0)
        d = net.copy(piece(kd, half, hi), dst.at[1, hi, :], p.dev(dy=-1))
        return u, d

    def plain_up(far, half, dst):
        return net.copy(piece(block(far, 1), half, hi), dst.at[0, hi, :], p.dev(dy=1))

    def plain_down(far, half, dst):
        return net.copy(piece(block(far, -1), half, lo), dst.at[1, lo, :], p.dev(dy=-1))

    z1, z2 = {}, {}

    def z_first(dy):
        k = block(True, dy)
        project(k, 1)
        z1[dy] = (
            net.copy(piece(k, 1, lo), tmpZ.at[dy % 4, 0], p.dev(dz=1)),
            net.copy(piece(k, 1, hi), tmpZ.at[dy % 4, 1], p.dev(dz=-1)),
        )

    def z_on(dy):
        got(z1[dy][0])
        a = net.copy(tmpZ.at[dy % 4, 0], rz.at[dy % 4, lo, :], p.dev(dz=1))
        got(z1[dy][1])
        b = net.copy(tmpZ.at[dy % 4, 1], rz.at[dy % 4, hi, :], p.dev(dz=-1))
        z2[dy] = (a, b)

    def z_add(dy):
        got(*z2[dy])
        add(block(False, dy), 1, 0, 8, rz.at[dy % 4], 0)

    def exchange(kind):
        return [net.copy(stage.at[kind], exch.at[kind, p.t], d) for d in teachers]

    def exchanged(kind, copies):
        exch[kind, p.t] = stage[kind]
        got(*copies)
        total = exch[kind, 0]
        for t in range(1, 8):
            total = total + exch[kind, t]
        return total

    z_first(2)
    project(block(True, 2), 0)
    open_far = open_to(block(True, 2), 0, r1.at[0])
    z_first(1)
    project(block(True, 1), 0)
    up_far = plain_up(True, 0, r2.at[0])
    project(block(True, -1), 0)
    down_far = plain_down(True, 0, r2.at[0])
    project(block(False, 2), 0)
    open_near = open_to(block(False, 2), 0, r1.at[1])
    z_on(2)
    z_first(-1)
    added_far = added(True, 0, open_far, r1.at[0], r2.at[0])
    z_on(1)
    z_first(0)
    project(block(False, 1), 0)
    up_near = plain_up(False, 0, r2.at[1])
    project(block(False, -1), 0)
    down_near = plain_down(False, 0, r2.at[1])
    for dy in (2, 1, -1, 0):
        project(block(False, dy), 1)
    k_far, k_near = block(True, 0), block(False, 0)
    project(k_far, 0)
    project(k_near, 0)
    got(cown[0][1], cown[1][0], *cfwd, cpart[0][1], cpart[1][0], *cfwd2)
    got(*dhop2[0], *dhop2[1], *dhop2[-1], *dhop2[2])
    got(*sfwd2["U"])
    ushared.append(share(U, s_index(2, True)))
    got(*ushared)

    def student(i, carry):
        rows = pl.ds(pl.multiple_of(i * 512, 512), 512)
        acc = sinv[rows, :].astype(F32)
        for t in range(8):
            w = bufU[2 * t : 2 * t + 2].reshape(256, 512)
            acc = acc + jnp.dot(bufC[t, rows, :], w, preferred_element_type=F32)
        ssq_out[rows, :] = fold(acc * acc)
        sres_out[rows, :] = acc
        return carry

    lax.fori_loop(0, 2, student, 0)
    to_rows(ssq_out, stage.at[1])
    ssums = exchange(1)

    net.sent(early)

    def turn(i, carry):
        t = div(i, 8)
        rows = pl.ds(pl.multiple_of(rem(i, 8) * 128, 128), 128)
        block = bufC[t, rows, :].astype(F32)
        at = pl.ds(pl.multiple_of(rem(t, 2) * 128, 128), 128)
        for core in range(2):
            turned = jnp.transpose(block[:, core * 128 : core * 128 + 128])
            bufW[core * 4 + div(t, 2), at, rows] = turned.astype(BF)
        return carry

    z_on(-1)
    z_add(2)
    opened = open_to(block(False, 2), 1, b1)
    added_near = added(False, 0, open_near, r1.at[1], r2.at[1])
    lax.fori_loop(0, 16, turn, 0)

    def three(k, half, src, i):
        at = pl.ds(pl.multiple_of(i * 128, 128), 128)
        own_part = bufA[k, at, columns(half)].astype(F32)
        return at, own_part + src[0, at, :].astype(F32) + src[1, at, :].astype(F32)

    got(up_far, down_far, *added_far)

    def far_sum(i, carry):
        at, total = three(k_far, 0, r2.at[0], i)
        zs[at, columns(0)] = total.astype(BF)
        return carry

    lax.fori_loop(0, 8, far_sum, 0)
    hop1 = (
        net.copy(zs.at[lo, columns(0)], tmpE.at[0], p.dev(dz=1)),
        net.copy(zs.at[hi, columns(0)], tmpE.at[1], p.dev(dz=-1)),
    )
    z_add(1)
    up_last = plain_up(False, 1, b2)
    z_on(0)
    to_rows(sq_out, stage.at[0])
    tsums = exchange(0)
    lax.fori_loop(16, 32, turn, 0)
    got(hop1[0])
    h2a = net.copy(tmpE.at[0], r3.at[lo, :], p.dev(dz=1))
    got(hop1[1])
    h2b = net.copy(tmpE.at[1], r3.at[hi, :], p.dev(dz=-1))
    z_add(-1)
    down_last = plain_down(False, 1, b2)
    added_last = added(False, 1, opened, b1, b2)
    lax.fori_loop(32, 48, turn, 0)
    to_columns(lax.rsqrt(exchanged(0, tsums) / DT + epsilon), sq_out)
    to_columns(lax.rsqrt(exchanged(1, ssums) / DS + epsilon), scol)
    got(up_near, down_near, *added_near)
    lax.fori_loop(48, 64, turn, 0)
    got(h2a, h2b)

    def near_sum(i, carry):
        at, total = three(k_near, 0, r2.at[1], i)
        total = total + r3[at, :].astype(F32)
        target[at, columns(0)] = (total * sq_out[at, 0:1]).astype(BF)
        return carry

    lax.fori_loop(0, 8, near_sum, 0)

    def send_rows(half):
        out = {}
        for group in (1, 2, 3, 0):
            rows = slice(group * 256, group * 256 + 256)
            picked = jnp.dot(
                pick[rows, :], target[:, columns(half)], preferred_element_type=F32
            ).astype(BF)
            tinv[rows, columns(half)] = picked
            if group == 0:
                frecv[p.s, :, columns(half)] = picked[0:64, :]
            for m in range(max(group * 4, 1), group * 4 + 4):
                out[m] = net.copy(
                    tinv.at[pl.ds(m * 64, 64), columns(half)],
                    frecv.at[p.s, :, columns(half)],
                    students[m - 1],
                )
        return out

    moved = send_rows(0)
    z_add(0)
    got(up_last, down_last, *added_last)

    def last_sum(i, carry):
        at, total = three(k_near, 1, b2, i)
        target[at, columns(1)] = (total * sq_out[at, 0:1]).astype(BF)
        return carry

    lax.fori_loop(0, 8, last_sum, 0)
    moved_last = send_rows(1)

    def compared(half, copies):
        cols = columns(half)
        gain_values = sgain[:, cols]
        partial = jnp.zeros((1, 256), F32)
        for m in (0, *range(4, 16), 1, 2, 3):
            if m:
                got(copies[m])
            b = rem(p.s + (16 - m), 16)
            rows = pl.ds(pl.multiple_of(b * 64, 64), 64)
            normed = sres_out[rows, cols] * scol[rows, 0:1]
            grad_out = (normed * gain_values - frecv[b, :, cols].astype(F32)) * lcol[rows, 0:1]
            partial = partial + jnp.sum(grad_out * normed, axis=0, keepdims=True)
            grad_norm = grad_out * gain_values
            gn[rows, cols] = grad_norm
            product = grad_norm * normed
            lanes = product[:, 0:128] + product[:, 128:256]
            ssq_out[rows, :] = lanes if half == 0 else ssq_out[rows, :] + lanes
        gstage[:, cols] = partial

    compared(0, moved)
    compared(1, moved_last)
    to_rows(ssq_out, stage.at[2])
    inner = exchange(2)
    gained = [net.copy(gstage, gains.at[p.s], d) for d in students]
    net.sent(hop1)
    to_columns(exchanged(2, inner) / DS, sq_out)

    def grad(i, carry):
        rows = pl.ds(pl.multiple_of(i * 128, 128), 128)
        scale = scol[rows, 0:1]
        normed = sres_out[rows, :] * scale
        zs[rows, :] = (scale * (gn[rows, :] - normed * sq_out[rows, 0:1])).astype(BF)
        return carry

    lax.fori_loop(0, 8, grad, 0)

    def product(core, i):
        return jnp.dot(bufW[core * 4 + i], zs[...], preferred_element_type=F32)

    halves = []
    for i in range(4):
        sinv[i * 256 : i * 256 + 256, :] = product(1 - p.core, i).astype(BF)
        part = pl.ds(i * 256, 256)
        halves.append(net.copy(sinv.at[part, :], sibr.at[part, :], sib))
    for i in range(4):
        own_part = product(p.core, i)
        got(halves[i])
        total = own_part + sibr[i * 256 : i * 256 + 256, :].astype(F32)
        tinv[i * 256 : i * 256 + 256, 512:1024] = total.astype(BF)
    chip = div(p.s, 2)
    parts = []
    for m in range(1, 8):
        q = rem(chip + m, 8)
        rows = pl.ds(pl.multiple_of(q * 128, 128), 128)
        to = {"teacher": p.t, "student": q * 2 + p.core}
        parts.append(net.copy(tinv.at[rows, right], grecv.at[m - 1], to))
    gains[p.s] = gstage[...]
    got(*gained)
    total_gain = gains[0]
    for b in range(1, 16):
        total_gain = total_gain + gains[b]
    gain_out[...] = total_gain
    total = tinv[pl.ds(pl.multiple_of(chip * 128, 128), 128), 512:1024].astype(F32)
    for m in range(7):
        got(parts[m])
        total = total + grecv[m].astype(F32)
    weight_out[...] = total
    net.finish()


def step(tin, tattn, tw, tgain, proj, sin, sattn, su, sgain, token_ids, row_order):
    anywhere = pl.BlockSpec(memory_space=pl.ANY)
    vmem = pl.BlockSpec(memory_space=pltpu.VMEM)
    V = pltpu.VMEM
    weight, gain = pl.pallas_call(
        step_kernel,
        out_shape=(
            jax.ShapeDtypeStruct((128, 512), F32),
            jax.ShapeDtypeStruct((1, 512), F32),
        ),
        in_specs=[anywhere] * 3 + [vmem] + [anywhere] * 4 + [vmem, anywhere, vmem],
        out_specs=(vmem, vmem),
        scratch_shapes=[
            V((8, 1024, 512), BF),
            V((8, 1024, 256), BF),
            V((16, 256, 1024), BF),
            V((16, 1024, 256), BF),
            V((16, 128, 512), BF),
            V((1024, 1024), BF),
            V((1024, 512), BF),
            V((1024, 1024), BF),
            V((1024, 1024), BF),
            V((2, 512, 512), BF),
            V((2, 512, 128), BF),
            V((4, 2, 512, 128), BF),
            V((2, 512, 256), BF),
            V((4, 2, 512, 256), BF),
            V((4, 1024, 256), BF),
            V((2, 2, 512, 256), BF),
            V((2, 2, 1024, 256), BF),
            V((2, 512, 256), BF),
            V((2, 1024, 256), BF),
            V((1024, 256), BF),
            V((1024, 512), BF),
            V((1024, 128), F32),
            V((1024, 512), F32),
            V((1024, 128), F32),
            V((1024, 512), BF),
            V((16, 64, 512), BF),
            V((1024, 512), F32),
            V((1024, 512), BF),
            V((7, 128, 512), BF),
            V((16, 8, 128), jnp.int32),
            V((4, 128, 128), F32),
            V((1024, 128), F32),
            V((1024, 128), F32),
            V((3, 8, 128), F32),
            V((3, 8, 8, 128), F32),
            V((1, 512), F32),
            V((16, 1, 512), F32),
            pltpu.SemaphoreType.DMA((SLOTS,)),
            pltpu.SemaphoreType.DMA((SLOTS,)),
            pltpu.SemaphoreType.DMA((16,)),
        ],
        compiler_params=pltpu.CompilerParams(
            collective_id=0, has_side_effects=True, vmem_limit_bytes=67043328
        ),
        name="step",
    )(
        tin, tattn, tw, tgain.astype(F32).reshape(1, -1), proj, sin, sattn, su,
        sgain.astype(F32).reshape(1, -1), token_ids.reshape(8, 128), row_order.reshape(128, 128),
    )
    return weight, gain.reshape(512)


def solution(mesh):
    placed = (
        P("student", "teacher"),
        P("student", "teacher"),
        P("student", "teacher"),
        P("teacher"),
        P("teacher", "student"),
        P("student", "teacher"),
        P("student", "teacher"),
        P("student", "teacher"),
        P("teacher"),
        P("student"),
        P(),
    )
    return jax.shard_map(
        step,
        mesh=mesh,
        in_specs=placed,
        out_specs=(P("student", "teacher"), P("teacher")),
        check_vma=False,
    )
```

```python
import math

import jax
import jax.numpy as jnp
from jax import lax
from jax.experimental import pallas as pl
from jax.experimental.pallas import tpu as pltpu
from jax.sharding import PartitionSpec as P

DT = 8192
DS = 4096
PAD_ID = 128004
epsilon = 1e-05

BF = jnp.bfloat16
F32 = jnp.float32
SLOTS = 256
LOSS = 1.0 / math.sqrt(16384)


def div(a, b):
    return lax.div(a, jnp.int32(b))


def rem(a, b):
    return lax.rem(a, jnp.int32(b))


class Place:
    def __init__(self):
        t = lax.axis_index("teacher")
        s = lax.axis_index("student")
        self.t, self.s = t, s
        self.zh, self.y = div(t, 4), rem(t, 4)
        self.zl, self.x, self.core = div(s, 8), rem(div(s, 2), 4), rem(s, 2)
        self.z = self.zh * 2 + self.zl

    def dev(self, dz=0, dy=0, dx=0, dc=0):
        t, s = self.index(dz, dy, dx, dc)
        return {"teacher": t, "student": s}

    def index(self, dz=0, dy=0, dx=0, dc=0):
        z, y, x, c = self.z, self.y, self.x, self.core
        if dz:
            z = rem(z + (dz % 4), 4)
        if dy:
            y = rem(y + (dy % 4), 4)
        if dx:
            x = rem(x + (dx % 4), 4)
        if dc:
            c = 1 - c
        return div(z, 2) * 4 + y, rem(z, 2) * 8 + x * 2 + c


class Net:
    def __init__(self, send, recv):
        self.send, self.recv, self.n, self.open = send, recv, 0, []

    def copy(self, src, dst, device):
        c = pltpu.make_async_remote_copy(
            src_ref=src,
            dst_ref=dst,
            send_sem=self.send.at[self.n],
            recv_sem=self.recv.at[self.n],
            device_id=device,
            device_id_type=pl.DeviceIdType.MESH,
        )
        self.n += 1
        c.start()
        self.open.append(c)
        return c

    def sent(self, copies):
        for c in copies:
            c.wait_send()
        gone = {id(c) for c in copies}
        self.open = [c for c in self.open if id(c) not in gone]

    def finish(self):
        for c in self.open:
            c.wait_send()
        self.open = []


def got(*copies):
    for c in copies:
        c.wait_recv()


def to_rows(lanes, out):
    for q in range(8):
        turned = jnp.transpose(lanes[q * 128 : q * 128 + 128, :])
        out[q : q + 1, :] = jnp.sum(turned, axis=0, keepdims=True)


def to_columns(rows, out):
    for q in range(8):
        wide = jnp.broadcast_to(rows[q : q + 1, :], (128, 128))
        out[q * 128 : q * 128 + 128, :] = jnp.transpose(wide)


def fold(a):
    return a[:, 0:128] + a[:, 128:256] + a[:, 256:384] + a[:, 384:512]


def step_kernel(
    tin, tattn, tw, tgain_in, proj, sin, sattn, su, sgain_in, tokens, order_in,
    weight_out, gain_out,
    bufA, bufC, bufW, bufP, bufU, tinv, sinv, hid,
    pick, tmpA, tmpC, tmpD, tmpE, tmpZ, rz, r1, r2, b1, b2, r3, zs,
    sq_out, sres_out, ssq_out, target, frecv, gn, sibr, grecv, tok, rowbuf,
    tgain, sgain, order, scol, lcol, stage, exch, gstage, gains,
    send, recv, local,
):
    p = Place()
    up, down = {"dy": 1}, {"dy": -1}
    barrier = pltpu.get_barrier_semaphore()
    teachers = [{"teacher": rem(p.t + j, 8), "student": p.s} for j in range(1, 8)]
    students = [{"teacher": p.t, "student": rem(p.s + j, 16)} for j in range(1, 16)]
    across = {"teacher": rem(p.t + 4, 8), "student": rem(p.s + 8, 16)}
    met = teachers + students + [across]
    for d in met:
        pl.semaphore_signal(barrier, inc=1, device_id=d, device_id_type=pl.DeviceIdType.MESH)
    pl.semaphore_wait(barrier, len(met))
    net = Net(send, recv)

    A = (tattn, bufA, tmpA, pl.ds(0, 512), 512)
    C = (sattn, bufC, tmpC, pl.ds(0, 128), 512)
    D = (sattn, bufC, tmpD, pl.ds(128, 128), 512)
    W = (tw, bufW, None, pl.ds(0, 1024), 128)
    Q = (proj, bufP, None, pl.ds(0, 256), 512)
    U = (su, bufU, None, pl.ds(0, 512), 64)

    def own(arr, h):
        half = arr[-1]
        return arr[0].at[pl.ds(h * half, half), arr[3]]

    def slot(arr, i, h):
        half = arr[-1]
        return arr[1].at[i, pl.ds(h * half, half), arr[3]]

    tp = p.index(dz=2)[0]
    zpart = {"teacher": p.t, "student": rem(p.s + 8, 16)}
    sp = rem(p.s + 8, 16)
    sib = p.dev(dc=1)
    sib_index = p.index(dc=1)[1]
    locals_ = []

    def bring(src, dst):
        c = pltpu.make_async_copy(src, dst, local.at[len(locals_)])
        c.start()
        locals_.append(c)
        return c

    def t_own(arr):
        ups = [net.copy(own(arr, h), slot(arr, p.t, h), p.dev(dy=1)) for h in (0, 1)]
        downs = [net.copy(own(arr, h), slot(arr, p.t, h), p.dev(dy=-1)) for h in (1, 0)][::-1]
        return ups, downs

    def t_hop1(arr):
        return [
            net.copy(own(arr, 0), arr[2].at[0], p.dev(dz=1)),
            net.copy(own(arr, 1), arr[2].at[1], p.dev(dz=-1)),
        ]

    def t_hop2(arr, hop1):
        got(hop1[0])
        a = net.copy(arr[2].at[0], slot(arr, p.index(dz=-1)[0], 0), p.dev(dz=1))
        got(hop1[1])
        b = net.copy(arr[2].at[1], slot(arr, p.index(dz=1)[0], 1), p.dev(dz=-1))
        return [a, b]

    def t_forward(arr, ups, downs, dz):
        got(ups[0])
        a = net.copy(slot(arr, p.index(dz=dz, dy=-1)[0], 0), slot(arr, p.index(dz=dz, dy=-1)[0], 0), p.dev(dy=1))
        got(downs[1])
        b = net.copy(slot(arr, p.index(dz=dz, dy=1)[0], 1), slot(arr, p.index(dz=dz, dy=1)[0], 1), p.dev(dy=-1))
        return [a, b]

    def t_partner(arr, hop2):
        got(*hop2)
        ups = [net.copy(slot(arr, tp, h), slot(arr, tp, h), p.dev(dy=1)) for h in (0, 1)]
        downs = [net.copy(slot(arr, tp, h), slot(arr, tp, h), p.dev(dy=-1)) for h in (1, 0)][::-1]
        return ups, downs

    def d_hop1(dy, halves=(0, 1)):
        out = []
        for h in halves:
            src = own(D, h) if dy == 0 else slot(D, p.index(dy=dy)[0], h)
            out.append(net.copy(src, tmpD.at[dy % 4, h], p.dev(dz=(1, -1)[h])))
        return out

    def d_hop2(dy, hop1):
        out = []
        for h, c in enumerate(hop1):
            got(c)
            at = slot(D, p.index(dz=(-1, 1)[h], dy=dy)[0], h)
            out.append(net.copy(tmpD.at[dy % 4, h], at, p.dev(dz=(1, -1)[h])))
        return out

    def s_own(arr):
        ups = [net.copy(own(arr, h), slot(arr, p.s, h), p.dev(dx=1)) for h in (0, 1)]
        downs = [net.copy(own(arr, h), slot(arr, p.s, h), p.dev(dx=-1)) for h in (1, 0)][::-1]
        return ups, downs

    def s_side(arr):
        return net.copy(arr[0], arr[1].at[p.s], zpart)

    def s_partner(arr, side):
        got(side)
        ups = [net.copy(slot(arr, sp, h), slot(arr, sp, h), p.dev(dx=1)) for h in (0, 1)]
        downs = [net.copy(slot(arr, sp, h), slot(arr, sp, h), p.dev(dx=-1)) for h in (1, 0)][::-1]
        return ups, downs

    def s_index(dx, other):
        i = p.index(dx=dx)[1]
        return rem(i + 8, 16) if other else i

    def s_forward(arr, ups, downs, other):
        got(ups[0])
        i = s_index(-1, other)
        a = net.copy(slot(arr, i, 0), slot(arr, i, 0), p.dev(dx=1))
        got(downs[1])
        j = s_index(1, other)
        b = net.copy(slot(arr, j, 1), slot(arr, j, 1), p.dev(dx=-1))
        return [a, b]

    def share(arr, i):
        return net.copy(arr[1].at[i], arr[1].at[i], sib)

    ssides, sowns, shared = {}, {}, []
    aown = t_own(A)
    ahop1 = t_hop1(A)
    for n, arr in (("W", W), ("Q", Q)):
        sowns[n] = s_own(arr)
        if n == "W":
            ssides[n] = s_side(arr)
        shared.append(net.copy(arr[0], arr[1].at[p.s], sib))
    bring(tattn, bufA.at[p.t])
    bring(tw, bufW.at[p.s])
    bring(proj, bufP.at[p.s])
    bring(tin, tinv)
    bring(sattn, bufC.at[p.t])
    bring(su, bufU.at[p.s])
    bring(sin, sinv)
    down_ = t_own(D)
    told = [net.copy(tokens, tok.at[p.s], d) for d in students]
    bring(tokens, tok.at[p.s])
    bring(tgain_in, tgain)
    bring(sgain_in, sgain)
    bring(order_in, order)
    sowns["U"] = s_own(U)
    shared.append(net.copy(U[0], U[1].at[p.s], sib))
    S = (("W", W), ("Q", Q), ("U", U))
    sfwd, sfwd2, sparts = {}, {}, {}

    ahop2 = t_hop2(A, ahop1)
    dhop1, dhop2 = {}, {}
    ssides["Q"] = s_side(Q)
    dhop1[0] = d_hop1(0)
    ssides["U"] = s_side(U)
    for n, arr in S[:2]:
        sfwd[n] = s_forward(arr, *sowns[n], False)
    afwd = t_forward(A, *aown, 0)
    sparts["W"] = s_partner(W, ssides["W"])
    dfwd = t_forward(D, *down_, 0)
    apart = t_partner(A, ahop2)
    got(down_[0][1], down_[1][0])
    dhop1[-1] = d_hop1(-1)
    dhop1[1] = d_hop1(1)
    dhop2[0] = d_hop2(0, dhop1[0])
    sparts["Q"] = s_partner(Q, ssides["Q"])
    for n, arr in S[:2]:
        got(sowns[n][0][1], sowns[n][1][0])
        shared.append(share(arr, sp))
        shared.append(share(arr, s_index(-1, False)))
        shared.append(share(arr, s_index(1, False)))
    sfwd["U"] = s_forward(U, *sowns["U"], False)
    sparts["U"] = s_partner(U, ssides["U"])
    dhop2[-1] = d_hop2(-1, dhop1[-1])
    dhop2[1] = d_hop2(1, dhop1[1])
    for n, arr in S[:2]:
        sfwd2[n] = s_forward(arr, *sparts[n], True)
    afwd2 = t_forward(A, *apart, 2)
    chop1 = t_hop1(C)
    got(*dfwd)
    dhop1[2] = d_hop1(2)
    cown = t_own(C)
    chop2 = t_hop2(C, chop1)
    dhop2[2] = d_hop2(2, dhop1[2])
    for n, arr in S[:2]:
        got(*sfwd[n], sparts[n][0][1], sparts[n][1][0])
        shared.append(share(arr, s_index(2, False)))
        shared.append(share(arr, s_index(-1, True)))
        shared.append(share(arr, s_index(1, True)))
    sfwd2["U"] = s_forward(U, *sparts["U"], True)
    got(sowns["U"][0][1], sowns["U"][1][0], sparts["U"][0][1], sparts["U"][1][0], *sfwd["U"])
    ushared = [
        share(U, sp),
        share(U, s_index(-1, False)),
        share(U, s_index(1, False)),
        share(U, s_index(2, False)),
        share(U, s_index(-1, True)),
        share(U, s_index(1, True)),
    ]
    for c in locals_:
        c.wait()

    wide = lax.broadcasted_iota(jnp.int32, (64, 1024), 1).astype(F32)
    narrow = lax.broadcasted_iota(jnp.int32, (64, 128), 1).astype(F32)
    rowbuf[...] = jnp.zeros_like(rowbuf)
    for m in range(16):
        b = rem(p.s + m, 16)
        rowbuf[0, m : m + 1, :] = order[pl.ds(b * 8 + div(p.s, 2), 1), :].astype(F32)
    rowbuf[1, 0:8, :] = order[pl.ds(pl.multiple_of(p.s * 8, 8), 8), :].astype(F32)
    for n in range(2):
        rowbuf[2 + n] = jnp.transpose(rowbuf[n])
    half = pl.ds(pl.multiple_of(rem(p.s, 2) * 64, 64), 64)
    base = (p.s * 1024).astype(F32)
    mine = rowbuf[2, half, :] - base
    for m in range(16):
        pick[m * 64 : m * 64 + 64, :] = jnp.where(wide == mine[:, m : m + 1], 1.0, 0.0).astype(BF)

    got(*told)
    for b in range(16):
        low = (b % 2) * 64
        named = rowbuf[3, low : low + 64, b // 2 : b // 2 + 1] - float(b * 1024)
        live = jnp.where(tok[b] != PAD_ID, LOSS, 0.0)
        acc = jnp.zeros((64, 128), F32)
        for q in range(8):
            acc = acc + jnp.where(narrow == named - float(q * 128), live[q : q + 1, :], 0.0)
        total = jnp.sum(acc, axis=1, keepdims=True)
        lcol[b * 64 : b * 64 + 64, :] = jnp.broadcast_to(total, (64, 128))

    for n, arr in S[:2]:
        got(*sfwd2[n])
        shared.append(share(arr, s_index(2, True)))
    got(aown[0][1], aown[1][0], *afwd, apart[0][1], apart[1][0], *afwd2)
    cfwd = t_forward(C, *cown, 0)
    cpart = t_partner(C, chop2)
    got(*shared)
    sq_out[...] = jnp.zeros_like(sq_out)

    def first(i, carry):
        rows = pl.ds(pl.multiple_of(div(i, 2) * 512, 512), 512)
        cols = pl.ds(pl.multiple_of(rem(i, 2) * 512, 512), 512)
        acc = tinv[rows, cols].astype(F32)
        for t in range(8):
            w = bufW[2 * t : 2 * t + 2, :, cols].reshape(512, 512)
            acc = acc + jnp.dot(bufA[t, rows, :], w, preferred_element_type=F32)
        square = acc * acc
        sq_out[rows, :] += square[:, 0:128] + square[:, 128:256] + square[:, 256:384] + square[:, 384:512]
        hid[rows, cols] = (acc * tgain[cols].astype(F32).reshape(1, 512)).astype(BF)
        return carry

    lax.fori_loop(0, 2, first, 0)
    cfwd2 = t_forward(C, *cpart, 2)
    lax.fori_loop(2, 4, first, 0)
    early = list(net.open)
    a_sends = [*aown[0], *aown[1], *ahop1, *ahop2, *afwd, *apart[0], *apart[1], *afwd2]
    net.sent(a_sends)
    gone = {id(c) for c in a_sends}
    early = [c for c in early if id(c) not in gone]

    def columns(half):
        return pl.ds(half * 256, 256)

    def project(k, half):
        def step(i, carry):
            rows = pl.ds(pl.multiple_of(i * 512, 512), 512)
            bufA[k, rows, columns(half)] = jnp.dot(
                hid[rows, :], bufP[2 * k + half], preferred_element_type=F32
            ).astype(BF)
            return carry

        lax.fori_loop(0, 2, step, 0)

    def block(far, dy):
        zh = 1 - p.zh if far else p.zh
        y = rem(p.y + (dy % 4), 4)
        return zh * 4 + y

    lo, hi = pl.ds(0, 512), pl.ds(512, 512)
    right = pl.ds(512, 512)

    def add(k, half, base, count, ref, rebase):
        def step(i, carry):
            at = pl.ds(pl.multiple_of(rebase + i * 128, 128), 128)
            rows = pl.ds(pl.multiple_of(base + i * 128, 128), 128)
            both = bufA[k, rows, columns(half)].astype(F32) + ref[at, :].astype(F32)
            bufA[k, rows, columns(half)] = both.astype(BF)
            return carry

        lax.fori_loop(0, count, step, 0)

    def piece(k, half, rows):
        return bufA.at[k, rows, columns(half)]

    def open_to(k, half, dst):
        return (
            net.copy(piece(k, half, lo), dst.at[0], p.dev(dy=1)),
            net.copy(piece(k, half, hi), dst.at[1], p.dev(dy=-1)),
        )

    def added(far, half, opened, src, dst):
        ku, kd = block(far, 1), block(far, -1)
        got(opened[0])
        add(ku, half, 0, 4, src.at[0], 0)
        u = net.copy(piece(ku, half, lo), dst.at[0, lo, :], p.dev(dy=1))
        got(opened[1])
        add(kd, half, 512, 4, src.at[1], 0)
        d = net.copy(piece(kd, half, hi), dst.at[1, hi, :], p.dev(dy=-1))
        return u, d

    def plain_up(far, half, dst):
        return net.copy(piece(block(far, 1), half, hi), dst.at[0, hi, :], p.dev(dy=1))

    def plain_down(far, half, dst):
        return net.copy(piece(block(far, -1), half, lo), dst.at[1, lo, :], p.dev(dy=-1))

    z1, z2 = {}, {}

    def z_first(dy):
        k = block(True, dy)
        project(k, 1)
        z1[dy] = (
            net.copy(piece(k, 1, lo), tmpZ.at[dy % 4, 0], p.dev(dz=1)),
            net.copy(piece(k, 1, hi), tmpZ.at[dy % 4, 1], p.dev(dz=-1)),
        )

    def z_on(dy):
        got(z1[dy][0])
        a = net.copy(tmpZ.at[dy % 4, 0], rz.at[dy % 4, lo, :], p.dev(dz=1))
        got(z1[dy][1])
        b = net.copy(tmpZ.at[dy % 4, 1], rz.at[dy % 4, hi, :], p.dev(dz=-1))
        z2[dy] = (a, b)

    def z_add(dy):
        got(*z2[dy])
        add(block(False, dy), 1, 0, 8, rz.at[dy % 4], 0)

    def exchange(kind):
        return [net.copy(stage.at[kind], exch.at[kind, p.t], d) for d in teachers]

    def exchanged(kind, copies):
        exch[kind, p.t] = stage[kind]
        got(*copies)
        total = exch[kind, 0]
        for t in range(1, 8):
            total = total + exch[kind, t]
        return total

    z_first(2)
    project(block(True, 2), 0)
    open_far = open_to(block(True, 2), 0, r1.at[0])
    z_first(1)
    project(block(True, 1), 0)
    up_far = plain_up(True, 0, r2.at[0])
    project(block(True, -1), 0)
    down_far = plain_down(True, 0, r2.at[0])
    project(block(False, 2), 0)
    open_near = open_to(block(False, 2), 0, r1.at[1])
    z_on(2)
    z_first(-1)
    added_far = added(True, 0, open_far, r1.at[0], r2.at[0])
    z_on(1)
    z_first(0)
    project(block(False, 1), 0)
    up_near = plain_up(False, 0, r2.at[1])
    project(block(False, -1), 0)
    down_near = plain_down(False, 0, r2.at[1])
    for dy in (2, 1, -1, 0):
        project(block(False, dy), 1)
    k_far, k_near = block(True, 0), block(False, 0)
    project(k_far, 0)
    project(k_near, 0)
    got(cown[0][1], cown[1][0], *cfwd, cpart[0][1], cpart[1][0], *cfwd2)
    got(*dhop2[0], *dhop2[1], *dhop2[-1], *dhop2[2])
    got(*sfwd2["U"])
    ushared.append(share(U, s_index(2, True)))
    got(*ushared)

    def student(i, carry):
        rows = pl.ds(pl.multiple_of(i * 512, 512), 512)
        acc = sinv[rows, :].astype(F32)
        for t in range(8):
            w = bufU[2 * t : 2 * t + 2].reshape(256, 512)
            acc = acc + jnp.dot(bufC[t, rows, :], w, preferred_element_type=F32)
        ssq_out[rows, :] = fold(acc * acc)
        sres_out[rows, :] = acc
        return carry

    lax.fori_loop(0, 2, student, 0)
    to_rows(ssq_out, stage.at[1])
    ssums = exchange(1)

    net.sent(early)

    def turn(i, carry):
        t = div(i, 8)
        rows = pl.ds(pl.multiple_of(rem(i, 8) * 128, 128), 128)
        block = bufC[t, rows, :].astype(F32)
        at = pl.ds(pl.multiple_of(rem(t, 2) * 128, 128), 128)
        for core in range(2):
            turned = jnp.transpose(block[:, core * 128 : core * 128 + 128])
            bufW[core * 4 + div(t, 2), at, rows] = turned.astype(BF)
        return carry

    z_on(-1)
    z_add(2)
    opened = open_to(block(False, 2), 1, b1)
    added_near = added(False, 0, open_near, r1.at[1], r2.at[1])
    lax.fori_loop(0, 16, turn, 0)

    def three(k, half, src, i):
        at = pl.ds(pl.multiple_of(i * 128, 128), 128)
        own_part = bufA[k, at, columns(half)].astype(F32)
        return at, own_part + src[0, at, :].astype(F32) + src[1, at, :].astype(F32)

    got(up_far, down_far, *added_far)

    def far_sum(i, carry):
        at, total = three(k_far, 0, r2.at[0], i)
        zs[at, columns(0)] = total.astype(BF)
        return carry

    lax.fori_loop(0, 8, far_sum, 0)
    hop1 = (
        net.copy(zs.at[lo, columns(0)], tmpE.at[0], p.dev(dz=1)),
        net.copy(zs.at[hi, columns(0)], tmpE.at[1], p.dev(dz=-1)),
    )
    z_add(1)
    up_last = plain_up(False, 1, b2)
    z_on(0)
    to_rows(sq_out, stage.at[0])
    tsums = exchange(0)
    lax.fori_loop(16, 32, turn, 0)
    got(hop1[0])
    h2a = net.copy(tmpE.at[0], r3.at[lo, :], p.dev(dz=1))
    got(hop1[1])
    h2b = net.copy(tmpE.at[1], r3.at[hi, :], p.dev(dz=-1))
    z_add(-1)
    down_last = plain_down(False, 1, b2)
    added_last = added(False, 1, opened, b1, b2)
    lax.fori_loop(32, 48, turn, 0)
    to_columns(lax.rsqrt(exchanged(0, tsums) / DT + epsilon), sq_out)
    to_columns(lax.rsqrt(exchanged(1, ssums) / DS + epsilon), scol)
    got(up_near, down_near, *added_near)
    lax.fori_loop(48, 64, turn, 0)
    got(h2a, h2b)

    def near_sum(i, carry):
        at, total = three(k_near, 0, r2.at[1], i)
        total = total + r3[at, :].astype(F32)
        target[at, columns(0)] = (total * sq_out[at, 0:1]).astype(BF)
        return carry

    lax.fori_loop(0, 8, near_sum, 0)

    def send_rows(half):
        out = {}
        for group in (1, 2, 3, 0):
            rows = slice(group * 256, group * 256 + 256)
            picked = jnp.dot(
                pick[rows, :], target[:, columns(half)], preferred_element_type=F32
            ).astype(BF)
            tinv[rows, columns(half)] = picked
            if group == 0:
                frecv[p.s, :, columns(half)] = picked[0:64, :]
            for m in range(max(group * 4, 1), group * 4 + 4):
                out[m] = net.copy(
                    tinv.at[pl.ds(m * 64, 64), columns(half)],
                    frecv.at[p.s, :, columns(half)],
                    students[m - 1],
                )
        return out

    moved = send_rows(0)
    z_add(0)
    got(up_last, down_last, *added_last)

    def last_sum(i, carry):
        at, total = three(k_near, 1, b2, i)
        target[at, columns(1)] = (total * sq_out[at, 0:1]).astype(BF)
        return carry

    lax.fori_loop(0, 8, last_sum, 0)
    moved_last = send_rows(1)

    def compared(half, copies):
        cols = columns(half)
        gain_values = sgain[cols].astype(F32).reshape(1, 256)
        partial = jnp.zeros((1, 256), F32)
        for m in (0, *range(4, 16), 1, 2, 3):
            if m:
                got(copies[m])
            b = rem(p.s + (16 - m), 16)
            rows = pl.ds(pl.multiple_of(b * 64, 64), 64)
            normed = sres_out[rows, cols] * scol[rows, 0:1]
            grad_out = (normed * gain_values - frecv[b, :, cols].astype(F32)) * lcol[rows, 0:1]
            partial = partial + jnp.sum(grad_out * normed, axis=0, keepdims=True)
            grad_norm = grad_out * gain_values
            gn[rows, cols] = grad_norm
            product = grad_norm * normed
            lanes = product[:, 0:128] + product[:, 128:256]
            ssq_out[rows, :] = lanes if half == 0 else ssq_out[rows, :] + lanes
        gstage[:, cols] = partial

    compared(0, moved)
    compared(1, moved_last)
    to_rows(ssq_out, stage.at[2])
    inner = exchange(2)
    gained = [net.copy(gstage, gains.at[p.s], d) for d in students]
    net.sent(hop1)
    to_columns(exchanged(2, inner) / DS, sq_out)

    def grad(i, carry):
        rows = pl.ds(pl.multiple_of(i * 128, 128), 128)
        scale = scol[rows, 0:1]
        normed = sres_out[rows, :] * scale
        zs[rows, :] = (scale * (gn[rows, :] - normed * sq_out[rows, 0:1])).astype(BF)
        return carry

    lax.fori_loop(0, 8, grad, 0)

    def product(core, i):
        return jnp.dot(bufW[core * 4 + i], zs[...], preferred_element_type=F32)

    halves = []
    for i in range(4):
        sinv[i * 256 : i * 256 + 256, :] = product(1 - p.core, i).astype(BF)
        part = pl.ds(i * 256, 256)
        halves.append(net.copy(sinv.at[part, :], sibr.at[part, :], sib))
    for i in range(4):
        own_part = product(p.core, i)
        got(halves[i])
        total = own_part + sibr[i * 256 : i * 256 + 256, :].astype(F32)
        tinv[i * 256 : i * 256 + 256, 512:1024] = total.astype(BF)
    chip = div(p.s, 2)
    parts = []
    for m in range(1, 8):
        q = rem(chip + m, 8)
        rows = pl.ds(pl.multiple_of(q * 128, 128), 128)
        to = {"teacher": p.t, "student": q * 2 + p.core}
        parts.append(net.copy(tinv.at[rows, right], grecv.at[m - 1], to))
    gains[p.s] = gstage[...]
    got(*gained)
    total_gain = gains[0]
    for b in range(1, 16):
        total_gain = total_gain + gains[b]
    gain_out[...] = total_gain
    total = tinv[pl.ds(pl.multiple_of(chip * 128, 128), 128), 512:1024].astype(F32)
    for m in range(7):
        got(parts[m])
        total = total + grecv[m].astype(F32)
    weight_out[...] = total
    net.finish()


def step(tin, tattn, tw, tgain, proj, sin, sattn, su, sgain, token_ids, row_order):
    anywhere = pl.BlockSpec(memory_space=pl.ANY)
    vmem = pl.BlockSpec(memory_space=pltpu.VMEM)
    V = pltpu.VMEM
    weight, gain = pl.pallas_call(
        step_kernel,
        out_shape=(
            jax.ShapeDtypeStruct((128, 512), F32),
            jax.ShapeDtypeStruct((1, 512), F32),
        ),
        in_specs=[anywhere] * 11,
        out_specs=(vmem, vmem),
        scratch_shapes=[
            V((8, 1024, 512), BF),
            V((8, 1024, 256), BF),
            V((16, 256, 1024), BF),
            V((16, 1024, 256), BF),
            V((16, 128, 512), BF),
            V((1024, 1024), BF),
            V((1024, 512), BF),
            V((1024, 1024), BF),
            V((1024, 1024), BF),
            V((2, 512, 512), BF),
            V((2, 512, 128), BF),
            V((4, 2, 512, 128), BF),
            V((2, 512, 256), BF),
            V((4, 2, 512, 256), BF),
            V((4, 1024, 256), BF),
            V((2, 2, 512, 256), BF),
            V((2, 2, 1024, 256), BF),
            V((2, 512, 256), BF),
            V((2, 1024, 256), BF),
            V((1024, 256), BF),
            V((1024, 512), BF),
            V((1024, 128), F32),
            V((1024, 512), F32),
            V((1024, 128), F32),
            V((1024, 512), BF),
            V((16, 64, 512), BF),
            V((1024, 512), F32),
            V((1024, 512), BF),
            V((7, 128, 512), BF),
            V((16, 8, 128), jnp.int32),
            V((4, 128, 128), F32),
            V((1024,), BF),
            V((512,), BF),
            V((128, 128), jnp.int32),
            V((1024, 128), F32),
            V((1024, 128), F32),
            V((3, 8, 128), F32),
            V((3, 8, 8, 128), F32),
            V((1, 512), F32),
            V((16, 1, 512), F32),
            pltpu.SemaphoreType.DMA((SLOTS,)),
            pltpu.SemaphoreType.DMA((SLOTS,)),
            pltpu.SemaphoreType.DMA((16,)),
        ],
        compiler_params=pltpu.CompilerParams(
            collective_id=0, has_side_effects=True, vmem_limit_bytes=67043328
        ),
        name="step",
    )(
        tin, tattn, tw, tgain, proj, sin, sattn, su,
        sgain, token_ids.reshape(8, 128), row_order.reshape(128, 128),
    )
    return weight, gain.reshape(512)


def solution(mesh):
    placed = (
        P("student", "teacher"),
        P("student", "teacher"),
        P("student", "teacher"),
        P("teacher"),
        P("teacher", "student"),
        P("student", "teacher"),
        P("student", "teacher"),
        P("student", "teacher"),
        P("teacher"),
        P("student"),
        P(),
    )
    return jax.shard_map(
        step,
        mesh=mesh,
        in_specs=placed,
        out_specs=(P("student", "teacher"), P("teacher")),
        check_vma=False,
    )
```

```python
import math

import jax
import jax.numpy as jnp
from jax import lax
from jax.experimental import pallas as pl
from jax.experimental.pallas import tpu as pltpu
from jax.sharding import PartitionSpec as P

DT = 8192
DS = 4096
PAD_ID = 128004
epsilon = 1e-05

BF = jnp.bfloat16
F32 = jnp.float32
SLOTS = 256
LOSS = 1.0 / math.sqrt(16384)


def div(a, b):
    return lax.div(a, jnp.int32(b))


def rem(a, b):
    return lax.rem(a, jnp.int32(b))


class Place:
    def __init__(self):
        t = lax.axis_index("teacher")
        s = lax.axis_index("student")
        self.t, self.s = t, s
        self.zh, self.y = div(t, 4), rem(t, 4)
        self.zl, self.x, self.core = div(s, 8), rem(div(s, 2), 4), rem(s, 2)
        self.z = self.zh * 2 + self.zl

    def dev(self, dz=0, dy=0, dx=0, dc=0):
        t, s = self.index(dz, dy, dx, dc)
        return {"teacher": t, "student": s}

    def index(self, dz=0, dy=0, dx=0, dc=0):
        z, y, x, c = self.z, self.y, self.x, self.core
        if dz:
            z = rem(z + (dz % 4), 4)
        if dy:
            y = rem(y + (dy % 4), 4)
        if dx:
            x = rem(x + (dx % 4), 4)
        if dc:
            c = 1 - c
        return div(z, 2) * 4 + y, rem(z, 2) * 8 + x * 2 + c


class Net:
    def __init__(self, send, recv):
        self.send, self.recv, self.n, self.open = send, recv, 0, []

    def copy(self, src, dst, device):
        c = pltpu.make_async_remote_copy(
            src_ref=src,
            dst_ref=dst,
            send_sem=self.send.at[self.n],
            recv_sem=self.recv.at[self.n],
            device_id=device,
            device_id_type=pl.DeviceIdType.MESH,
        )
        self.n += 1
        c.start()
        self.open.append(c)
        return c

    def sent(self, copies):
        for c in copies:
            c.wait_send()
        gone = {id(c) for c in copies}
        self.open = [c for c in self.open if id(c) not in gone]

    def finish(self):
        for c in self.open:
            c.wait_send()
        self.open = []


def got(*copies):
    for c in copies:
        c.wait_recv()


def to_rows(lanes, out):
    for q in range(8):
        turned = jnp.transpose(lanes[q * 128 : q * 128 + 128, :])
        out[q : q + 1, :] = jnp.sum(turned, axis=0, keepdims=True)


def to_columns(rows, out):
    for q in range(8):
        wide = jnp.broadcast_to(rows[q : q + 1, :], (128, 128))
        out[q * 128 : q * 128 + 128, :] = jnp.transpose(wide)


def fold(a):
    return a[:, 0:128] + a[:, 128:256] + a[:, 256:384] + a[:, 384:512]


def step_kernel(
    tin, tattn, tw, tgain_in, proj, sin, sattn, su, sgain_in, tokens, order_in,
    weight_out, gain_out,
    bufA, bufC, bufW, bufP, bufU, tinv, sinv, hid,
    pick, tmpA, tmpC, tmpD, tmpE, tmpZ, rz, r1, r2, b1, b2, r3, zs,
    sq_out, sres_out, ssq_out, target, frecv, gn, sibr, grecv, tok, rowbuf,
    tgain, sgain, order, scol, lcol, stage, exch, gstage, gains,
    send, recv, local,
):
    p = Place()
    up, down = {"dy": 1}, {"dy": -1}
    barrier = pltpu.get_barrier_semaphore()
    teachers = [{"teacher": rem(p.t + j, 8), "student": p.s} for j in range(1, 8)]
    students = [{"teacher": p.t, "student": rem(p.s + j, 16)} for j in range(1, 16)]
    across = {"teacher": rem(p.t + 4, 8), "student": rem(p.s + 8, 16)}
    met = teachers + students + [across]
    for d in met:
        pl.semaphore_signal(barrier, inc=1, device_id=d, device_id_type=pl.DeviceIdType.MESH)
    pl.semaphore_wait(barrier, len(met))
    net = Net(send, recv)

    A = (tattn, bufA, tmpA, pl.ds(0, 512), 512)
    C = (sattn, bufC, tmpC, pl.ds(0, 128), 512)
    D = (sattn, bufC, tmpD, pl.ds(128, 128), 512)
    W = (tw, bufW, None, pl.ds(0, 1024), 128)
    Q = (proj, bufP, None, pl.ds(0, 256), 512)
    U = (su, bufU, None, pl.ds(0, 512), 64)

    def own(arr, h):
        half = arr[-1]
        return arr[0].at[pl.ds(h * half, half), arr[3]]

    def slot(arr, i, h):
        half = arr[-1]
        return arr[1].at[i, pl.ds(h * half, half), arr[3]]

    tp = p.index(dz=2)[0]
    zpart = {"teacher": p.t, "student": rem(p.s + 8, 16)}
    sp = rem(p.s + 8, 16)
    sib = p.dev(dc=1)
    sib_index = p.index(dc=1)[1]
    locals_ = []

    def bring(src, dst):
        c = pltpu.make_async_copy(src, dst, local.at[len(locals_)])
        c.start()
        locals_.append(c)
        return c

    def t_own(arr):
        ups = [net.copy(own(arr, h), slot(arr, p.t, h), p.dev(dy=1)) for h in (0, 1)]
        downs = [net.copy(own(arr, h), slot(arr, p.t, h), p.dev(dy=-1)) for h in (1, 0)][::-1]
        return ups, downs

    def t_hop1(arr):
        return [
            net.copy(own(arr, 0), arr[2].at[0], p.dev(dz=1)),
            net.copy(own(arr, 1), arr[2].at[1], p.dev(dz=-1)),
        ]

    def t_hop2(arr, hop1):
        got(hop1[0])
        a = net.copy(arr[2].at[0], slot(arr, p.index(dz=-1)[0], 0), p.dev(dz=1))
        got(hop1[1])
        b = net.copy(arr[2].at[1], slot(arr, p.index(dz=1)[0], 1), p.dev(dz=-1))
        return [a, b]

    def t_forward(arr, ups, downs, dz):
        got(ups[0])
        a = net.copy(slot(arr, p.index(dz=dz, dy=-1)[0], 0), slot(arr, p.index(dz=dz, dy=-1)[0], 0), p.dev(dy=1))
        got(downs[1])
        b = net.copy(slot(arr, p.index(dz=dz, dy=1)[0], 1), slot(arr, p.index(dz=dz, dy=1)[0], 1), p.dev(dy=-1))
        return [a, b]

    def t_partner(arr, hop2):
        got(*hop2)
        ups = [net.copy(slot(arr, tp, h), slot(arr, tp, h), p.dev(dy=1)) for h in (0, 1)]
        downs = [net.copy(slot(arr, tp, h), slot(arr, tp, h), p.dev(dy=-1)) for h in (1, 0)][::-1]
        return ups, downs

    def d_hop1(dy, halves=(0, 1)):
        out = []
        for h in halves:
            src = own(D, h) if dy == 0 else slot(D, p.index(dy=dy)[0], h)
            out.append(net.copy(src, tmpD.at[dy % 4, h], p.dev(dz=(1, -1)[h])))
        return out

    def d_hop2(dy, hop1):
        out = []
        for h, c in enumerate(hop1):
            got(c)
            at = slot(D, p.index(dz=(-1, 1)[h], dy=dy)[0], h)
            out.append(net.copy(tmpD.at[dy % 4, h], at, p.dev(dz=(1, -1)[h])))
        return out

    def s_own(arr):
        ups = [net.copy(own(arr, h), slot(arr, p.s, h), p.dev(dx=1)) for h in (0, 1)]
        downs = [net.copy(own(arr, h), slot(arr, p.s, h), p.dev(dx=-1)) for h in (1, 0)][::-1]
        return ups, downs

    def s_side(arr):
        return net.copy(arr[0], arr[1].at[p.s], zpart)

    def s_partner(arr, side):
        got(side)
        ups = [net.copy(slot(arr, sp, h), slot(arr, sp, h), p.dev(dx=1)) for h in (0, 1)]
        downs = [net.copy(slot(arr, sp, h), slot(arr, sp, h), p.dev(dx=-1)) for h in (1, 0)][::-1]
        return ups, downs

    def s_index(dx, other):
        i = p.index(dx=dx)[1]
        return rem(i + 8, 16) if other else i

    def s_forward(arr, ups, downs, other):
        got(ups[0])
        i = s_index(-1, other)
        a = net.copy(slot(arr, i, 0), slot(arr, i, 0), p.dev(dx=1))
        got(downs[1])
        j = s_index(1, other)
        b = net.copy(slot(arr, j, 1), slot(arr, j, 1), p.dev(dx=-1))
        return [a, b]

    def share(arr, i):
        return net.copy(arr[1].at[i], arr[1].at[i], sib)

    ssides, sowns, shared = {}, {}, []
    aown = t_own(A)
    ahop1 = t_hop1(A)
    for n, arr in (("W", W), ("Q", Q)):
        sowns[n] = s_own(arr)
        if n == "W":
            ssides[n] = s_side(arr)
        shared.append(net.copy(arr[0], arr[1].at[p.s], sib))
    bring(tattn, bufA.at[p.t])
    bring(tw, bufW.at[p.s])
    bring(proj, bufP.at[p.s])
    bring(tin, tinv)
    bring(sattn, bufC.at[p.t])
    bring(su, bufU.at[p.s])
    bring(sin, sinv)
    down_ = t_own(D)
    told = [net.copy(tokens, tok.at[p.s], d) for d in students]
    bring(tokens, tok.at[p.s])
    bring(tgain_in, tgain)
    bring(sgain_in, sgain)
    bring(order_in, order)
    sowns["U"] = s_own(U)
    shared.append(net.copy(U[0], U[1].at[p.s], sib))
    S = (("W", W), ("Q", Q), ("U", U))
    sfwd, sfwd2, sparts = {}, {}, {}

    ahop2 = t_hop2(A, ahop1)
    dhop1, dhop2 = {}, {}
    ssides["Q"] = s_side(Q)
    dhop1[0] = d_hop1(0)
    ssides["U"] = s_side(U)
    for n, arr in S[:2]:
        sfwd[n] = s_forward(arr, *sowns[n], False)
    afwd = t_forward(A, *aown, 0)
    sparts["W"] = s_partner(W, ssides["W"])
    dfwd = t_forward(D, *down_, 0)
    apart = t_partner(A, ahop2)
    got(down_[0][1], down_[1][0])
    dhop1[-1] = d_hop1(-1)
    dhop1[1] = d_hop1(1)
    dhop2[0] = d_hop2(0, dhop1[0])
    sparts["Q"] = s_partner(Q, ssides["Q"])
    for n, arr in S[:2]:
        got(sowns[n][0][1], sowns[n][1][0])
        shared.append(share(arr, sp))
        shared.append(share(arr, s_index(-1, False)))
        shared.append(share(arr, s_index(1, False)))
    sfwd["U"] = s_forward(U, *sowns["U"], False)
    sparts["U"] = s_partner(U, ssides["U"])
    dhop2[-1] = d_hop2(-1, dhop1[-1])
    dhop2[1] = d_hop2(1, dhop1[1])
    for n, arr in S[:2]:
        sfwd2[n] = s_forward(arr, *sparts[n], True)
    afwd2 = t_forward(A, *apart, 2)
    chop1 = t_hop1(C)
    got(*dfwd)
    dhop1[2] = d_hop1(2)
    cown = t_own(C)
    chop2 = t_hop2(C, chop1)
    dhop2[2] = d_hop2(2, dhop1[2])
    for n, arr in S[:2]:
        got(*sfwd[n], sparts[n][0][1], sparts[n][1][0])
        shared.append(share(arr, s_index(2, False)))
        shared.append(share(arr, s_index(-1, True)))
        shared.append(share(arr, s_index(1, True)))
    sfwd2["U"] = s_forward(U, *sparts["U"], True)
    got(sowns["U"][0][1], sowns["U"][1][0], sparts["U"][0][1], sparts["U"][1][0], *sfwd["U"])
    ushared = [
        share(U, sp),
        share(U, s_index(-1, False)),
        share(U, s_index(1, False)),
        share(U, s_index(2, False)),
        share(U, s_index(-1, True)),
        share(U, s_index(1, True)),
    ]
    for c in locals_:
        c.wait()

    wide = lax.broadcasted_iota(jnp.int32, (64, 1024), 1).astype(F32)
    narrow = lax.broadcasted_iota(jnp.int32, (64, 128), 1).astype(F32)
    rowbuf[...] = jnp.zeros_like(rowbuf)
    for m in range(16):
        b = rem(p.s + m, 16)
        rowbuf[0, m : m + 1, :] = order[pl.ds(b * 8 + div(p.s, 2), 1), :].astype(F32)
    rowbuf[1, 0:8, :] = order[pl.ds(pl.multiple_of(p.s * 8, 8), 8), :].astype(F32)
    for n in range(2):
        rowbuf[2 + n] = jnp.transpose(rowbuf[n])
    half = pl.ds(pl.multiple_of(rem(p.s, 2) * 64, 64), 64)
    base = (p.s * 1024).astype(F32)
    mine = rowbuf[2, half, :] - base
    for m in range(16):
        pick[m * 64 : m * 64 + 64, :] = jnp.where(wide == mine[:, m : m + 1], 1.0, 0.0).astype(BF)

    got(*told)
    for b in range(16):
        low = (b % 2) * 64
        named = rowbuf[3, low : low + 64, b // 2 : b // 2 + 1] - float(b * 1024)
        live = jnp.where(tok[b] != PAD_ID, LOSS, 0.0)
        acc = jnp.zeros((64, 128), F32)
        for q in range(8):
            acc = acc + jnp.where(narrow == named - float(q * 128), live[q : q + 1, :], 0.0)
        total = jnp.sum(acc, axis=1, keepdims=True)
        lcol[b * 64 : b * 64 + 64, :] = jnp.broadcast_to(total, (64, 128))

    for n, arr in S[:2]:
        got(*sfwd2[n])
        shared.append(share(arr, s_index(2, True)))
    got(aown[0][1], aown[1][0], *afwd, apart[0][1], apart[1][0], *afwd2)
    cfwd = t_forward(C, *cown, 0)
    cpart = t_partner(C, chop2)
    got(*shared)
    sq_out[...] = jnp.zeros_like(sq_out)

    def first(i, carry):
        rows = pl.ds(pl.multiple_of(div(i, 2) * 512, 512), 512)
        cols = pl.ds(pl.multiple_of(rem(i, 2) * 512, 512), 512)
        acc = tinv[rows, cols].astype(F32)
        for t in range(8):
            w = bufW[2 * t : 2 * t + 2, :, cols].reshape(512, 512)
            acc = acc + jnp.dot(bufA[t, rows, :], w, preferred_element_type=F32)
        square = acc * acc
        sq_out[rows, :] += square[:, 0:128] + square[:, 128:256] + square[:, 256:384] + square[:, 384:512]
        hid[rows, cols] = (acc * tgain[cols].astype(F32).reshape(1, 512)).astype(BF)
        return carry

    lax.fori_loop(0, 2, first, 0)
    cfwd2 = t_forward(C, *cpart, 2)
    lax.fori_loop(2, 4, first, 0)
    early = list(net.open)
    a_sends = [*aown[0], *aown[1], *ahop1, *ahop2, *afwd, *apart[0], *apart[1], *afwd2]
    net.sent(a_sends)
    gone = {id(c) for c in a_sends}
    early = [c for c in early if id(c) not in gone]

    def columns(half):
        return pl.ds(half * 256, 256)

    def project(k, half):
        def step(i, carry):
            rows = pl.ds(pl.multiple_of(i * 512, 512), 512)
            bufA[k, rows, columns(half)] = jnp.dot(
                hid[rows, :], bufP[2 * k + half], preferred_element_type=F32
            ).astype(BF)
            return carry

        lax.fori_loop(0, 2, step, 0)

    def block(far, dy):
        zh = 1 - p.zh if far else p.zh
        y = rem(p.y + (dy % 4), 4)
        return zh * 4 + y

    lo, hi = pl.ds(0, 512), pl.ds(512, 512)
    right = pl.ds(512, 512)

    def add(k, half, base, count, ref, rebase):
        def step(i, carry):
            at = pl.ds(pl.multiple_of(rebase + i * 128, 128), 128)
            rows = pl.ds(pl.multiple_of(base + i * 128, 128), 128)
            both = bufA[k, rows, columns(half)].astype(F32) + ref[at, :].astype(F32)
            bufA[k, rows, columns(half)] = both.astype(BF)
            return carry

        lax.fori_loop(0, count, step, 0)

    def piece(k, half, rows):
        return bufA.at[k, rows, columns(half)]

    def open_to(k, half, dst):
        return (
            net.copy(piece(k, half, lo), dst.at[0], p.dev(dy=1)),
            net.copy(piece(k, half, hi), dst.at[1], p.dev(dy=-1)),
        )

    def added(far, half, opened, src, dst):
        ku, kd = block(far, 1), block(far, -1)
        got(opened[0])
        add(ku, half, 0, 4, src.at[0], 0)
        u = net.copy(piece(ku, half, lo), dst.at[0, lo, :], p.dev(dy=1))
        got(opened[1])
        add(kd, half, 512, 4, src.at[1], 0)
        d = net.copy(piece(kd, half, hi), dst.at[1, hi, :], p.dev(dy=-1))
        return u, d

    def plain_up(far, half, dst):
        return net.copy(piece(block(far, 1), half, hi), dst.at[0, hi, :], p.dev(dy=1))

    def plain_down(far, half, dst):
        return net.copy(piece(block(far, -1), half, lo), dst.at[1, lo, :], p.dev(dy=-1))

    z1, z2 = {}, {}

    def z_first(dy):
        k = block(True, dy)
        project(k, 1)
        z1[dy] = (
            net.copy(piece(k, 1, lo), tmpZ.at[dy % 4, 0], p.dev(dz=1)),
            net.copy(piece(k, 1, hi), tmpZ.at[dy % 4, 1], p.dev(dz=-1)),
        )

    def z_on(dy):
        got(z1[dy][0])
        a = net.copy(tmpZ.at[dy % 4, 0], rz.at[dy % 4, lo, :], p.dev(dz=1))
        got(z1[dy][1])
        b = net.copy(tmpZ.at[dy % 4, 1], rz.at[dy % 4, hi, :], p.dev(dz=-1))
        z2[dy] = (a, b)

    def z_add(dy):
        got(*z2[dy])
        add(block(False, dy), 1, 0, 8, rz.at[dy % 4], 0)

    def exchange(kind):
        return [net.copy(stage.at[kind], exch.at[kind, p.t], d) for d in teachers]

    def exchanged(kind, copies):
        exch[kind, p.t] = stage[kind]
        got(*copies)
        total = exch[kind, 0]
        for t in range(1, 8):
            total = total + exch[kind, t]
        return total

    z_first(2)
    project(block(True, 2), 0)
    open_far = open_to(block(True, 2), 0, r1.at[0])
    z_first(1)
    project(block(True, 1), 0)
    up_far = plain_up(True, 0, r2.at[0])
    project(block(True, -1), 0)
    down_far = plain_down(True, 0, r2.at[0])
    project(block(False, 2), 0)
    open_near = open_to(block(False, 2), 0, r1.at[1])
    z_on(2)
    z_first(-1)
    added_far = added(True, 0, open_far, r1.at[0], r2.at[0])
    z_on(1)
    project(block(False, 1), 0)
    up_near = plain_up(False, 0, r2.at[1])
    project(block(False, -1), 0)
    down_near = plain_down(False, 0, r2.at[1])
    for dy in (2, 1, -1, 0):
        project(block(False, dy), 1)
    k_far, k_near = block(True, 0), block(False, 0)
    project(k_far, 0)
    project(k_near, 0)
    z_on(-1)
    z_first(0)
    z_add(2)
    opened = open_to(block(False, 2), 1, b1)
    added_near = added(False, 0, open_near, r1.at[1], r2.at[1])
    got(cown[0][1], cown[1][0], *cfwd, cpart[0][1], cpart[1][0], *cfwd2)
    got(*dhop2[0], *dhop2[1], *dhop2[-1], *dhop2[2])
    got(*sfwd2["U"])
    ushared.append(share(U, s_index(2, True)))
    got(*ushared)

    def student(i, carry):
        rows = pl.ds(pl.multiple_of(i * 512, 512), 512)
        acc = sinv[rows, :].astype(F32)
        for t in range(8):
            w = bufU[2 * t : 2 * t + 2].reshape(256, 512)
            acc = acc + jnp.dot(bufC[t, rows, :], w, preferred_element_type=F32)
        ssq_out[rows, :] = fold(acc * acc)
        sres_out[rows, :] = acc
        return carry

    lax.fori_loop(0, 2, student, 0)
    to_rows(ssq_out, stage.at[1])
    ssums = exchange(1)

    net.sent(early)

    def turn(i, carry):
        t = div(i, 8)
        rows = pl.ds(pl.multiple_of(rem(i, 8) * 128, 128), 128)
        block = bufC[t, rows, :].astype(F32)
        at = pl.ds(pl.multiple_of(rem(t, 2) * 128, 128), 128)
        for core in range(2):
            turned = jnp.transpose(block[:, core * 128 : core * 128 + 128])
            bufW[core * 4 + div(t, 2), at, rows] = turned.astype(BF)
        return carry

    lax.fori_loop(0, 16, turn, 0)

    def three(k, half, src, i):
        at = pl.ds(pl.multiple_of(i * 128, 128), 128)
        own_part = bufA[k, at, columns(half)].astype(F32)
        return at, own_part + src[0, at, :].astype(F32) + src[1, at, :].astype(F32)

    got(up_far, down_far, *added_far)

    def far_sum(i, carry):
        at, total = three(k_far, 0, r2.at[0], i)
        zs[at, columns(0)] = total.astype(BF)
        return carry

    lax.fori_loop(0, 8, far_sum, 0)
    hop1 = (
        net.copy(zs.at[lo, columns(0)], tmpE.at[0], p.dev(dz=1)),
        net.copy(zs.at[hi, columns(0)], tmpE.at[1], p.dev(dz=-1)),
    )
    z_add(1)
    up_last = plain_up(False, 1, b2)
    z_on(0)
    to_rows(sq_out, stage.at[0])
    tsums = exchange(0)
    lax.fori_loop(16, 32, turn, 0)
    got(hop1[0])
    h2a = net.copy(tmpE.at[0], r3.at[lo, :], p.dev(dz=1))
    got(hop1[1])
    h2b = net.copy(tmpE.at[1], r3.at[hi, :], p.dev(dz=-1))
    z_add(-1)
    down_last = plain_down(False, 1, b2)
    added_last = added(False, 1, opened, b1, b2)
    lax.fori_loop(32, 48, turn, 0)
    to_columns(lax.rsqrt(exchanged(0, tsums) / DT + epsilon), sq_out)
    to_columns(lax.rsqrt(exchanged(1, ssums) / DS + epsilon), scol)
    got(up_near, down_near, *added_near)
    lax.fori_loop(48, 64, turn, 0)
    got(h2a, h2b)

    def near_sum(i, carry):
        at, total = three(k_near, 0, r2.at[1], i)
        total = total + r3[at, :].astype(F32)
        target[at, columns(0)] = (total * sq_out[at, 0:1]).astype(BF)
        return carry

    lax.fori_loop(0, 8, near_sum, 0)

    def send_rows(half):
        out = {}
        for group in (1, 2, 3, 0):
            rows = slice(group * 256, group * 256 + 256)
            picked = jnp.dot(
                pick[rows, :], target[:, columns(half)], preferred_element_type=F32
            ).astype(BF)
            tinv[rows, columns(half)] = picked
            if group == 0:
                frecv[p.s, :, columns(half)] = picked[0:64, :]
            for m in range(max(group * 4, 1), group * 4 + 4):
                out[m] = net.copy(
                    tinv.at[pl.ds(m * 64, 64), columns(half)],
                    frecv.at[p.s, :, columns(half)],
                    students[m - 1],
                )
        return out

    moved = send_rows(0)
    z_add(0)
    got(up_last, down_last, *added_last)

    def last_sum(i, carry):
        at, total = three(k_near, 1, b2, i)
        target[at, columns(1)] = (total * sq_out[at, 0:1]).astype(BF)
        return carry

    lax.fori_loop(0, 8, last_sum, 0)
    moved_last = send_rows(1)

    def compared(half, copies):
        cols = columns(half)
        gain_values = sgain[cols].astype(F32).reshape(1, 256)
        partial = jnp.zeros((1, 256), F32)
        for m in (0, *range(4, 16), 1, 2, 3):
            if m:
                got(copies[m])
            b = rem(p.s + (16 - m), 16)
            rows = pl.ds(pl.multiple_of(b * 64, 64), 64)
            normed = sres_out[rows, cols] * scol[rows, 0:1]
            grad_out = (normed * gain_values - frecv[b, :, cols].astype(F32)) * lcol[rows, 0:1]
            partial = partial + jnp.sum(grad_out * normed, axis=0, keepdims=True)
            grad_norm = grad_out * gain_values
            gn[rows, cols] = grad_norm
            product = grad_norm * normed
            lanes = product[:, 0:128] + product[:, 128:256]
            ssq_out[rows, :] = lanes if half == 0 else ssq_out[rows, :] + lanes
        gstage[:, cols] = partial

    compared(0, moved)
    compared(1, moved_last)
    to_rows(ssq_out, stage.at[2])
    inner = exchange(2)
    gained = [net.copy(gstage, gains.at[p.s], d) for d in students]
    net.sent(hop1)
    to_columns(exchanged(2, inner) / DS, sq_out)

    def grad(i, carry):
        rows = pl.ds(pl.multiple_of(i * 128, 128), 128)
        scale = scol[rows, 0:1]
        normed = sres_out[rows, :] * scale
        zs[rows, :] = (scale * (gn[rows, :] - normed * sq_out[rows, 0:1])).astype(BF)
        return carry

    lax.fori_loop(0, 8, grad, 0)

    def product(core, i):
        return jnp.dot(bufW[core * 4 + i], zs[...], preferred_element_type=F32)

    halves = {}
    for j in (2, 3, 1, 0):
        i = rem(div(p.s, 4) + j, 4)
        part = pl.ds(pl.multiple_of(i * 256, 256), 256)
        sinv[part, :] = product(1 - p.core, i).astype(BF)
        halves[j] = net.copy(sinv.at[part, :], sibr.at[part, :], sib)
    chip = div(p.s, 2)
    parts = []
    for j in (2, 3, 1, 0):
        i = rem(div(chip, 2) + j, 4)
        own_part = product(p.core, i)
        rows = pl.ds(pl.multiple_of(i * 256, 256), 256)
        got(halves[j])
        total = own_part + sibr[rows, :].astype(F32)
        tinv[rows, 512:1024] = total.astype(BF)
        for n in range(2):
            if j == 0 and n == 1:
                continue
            if j == 0:
                q = i * 2 + 1 - rem(chip, 2)
            else:
                q = i * 2 + rem(chip + n, 2)
            sub_rows = pl.ds(pl.multiple_of(q * 128, 128), 128)
            to = {"teacher": p.t, "student": q * 2 + p.core}
            parts.append(net.copy(tinv.at[sub_rows, right], grecv.at[len(parts)], to))
    gains[p.s] = gstage[...]
    got(*gained)
    total_gain = gains[0]
    for b in range(1, 16):
        total_gain = total_gain + gains[b]
    gain_out[...] = total_gain
    total = tinv[pl.ds(pl.multiple_of(chip * 128, 128), 128), 512:1024].astype(F32)
    for m in range(7):
        got(parts[m])
        total = total + grecv[m].astype(F32)
    weight_out[...] = total
    net.finish()


def step(tin, tattn, tw, tgain, proj, sin, sattn, su, sgain, token_ids, row_order):
    anywhere = pl.BlockSpec(memory_space=pl.ANY)
    vmem = pl.BlockSpec(memory_space=pltpu.VMEM)
    V = pltpu.VMEM
    weight, gain = pl.pallas_call(
        step_kernel,
        out_shape=(
            jax.ShapeDtypeStruct((128, 512), F32),
            jax.ShapeDtypeStruct((1, 512), F32),
        ),
        in_specs=[anywhere] * 11,
        out_specs=(vmem, vmem),
        scratch_shapes=[
            V((8, 1024, 512), BF),
            V((8, 1024, 256), BF),
            V((16, 256, 1024), BF),
            V((16, 1024, 256), BF),
            V((16, 128, 512), BF),
            V((1024, 1024), BF),
            V((1024, 512), BF),
            V((1024, 1024), BF),
            V((1024, 1024), BF),
            V((2, 512, 512), BF),
            V((2, 512, 128), BF),
            V((4, 2, 512, 128), BF),
            V((2, 512, 256), BF),
            V((4, 2, 512, 256), BF),
            V((4, 1024, 256), BF),
            V((2, 2, 512, 256), BF),
            V((2, 2, 1024, 256), BF),
            V((2, 512, 256), BF),
            V((2, 1024, 256), BF),
            V((1024, 256), BF),
            V((1024, 512), BF),
            V((1024, 128), F32),
            V((1024, 512), F32),
            V((1024, 128), F32),
            V((1024, 512), BF),
            V((16, 64, 512), BF),
            V((1024, 512), F32),
            V((1024, 512), BF),
            V((7, 128, 512), BF),
            V((16, 8, 128), jnp.int32),
            V((4, 128, 128), F32),
            V((1024,), BF),
            V((512,), BF),
            V((128, 128), jnp.int32),
            V((1024, 128), F32),
            V((1024, 128), F32),
            V((3, 8, 128), F32),
            V((3, 8, 8, 128), F32),
            V((1, 512), F32),
            V((16, 1, 512), F32),
            pltpu.SemaphoreType.DMA((SLOTS,)),
            pltpu.SemaphoreType.DMA((SLOTS,)),
            pltpu.SemaphoreType.DMA((16,)),
        ],
        compiler_params=pltpu.CompilerParams(
            collective_id=0, has_side_effects=True, vmem_limit_bytes=67043328
        ),
        name="step",
    )(
        tin, tattn, tw, tgain, proj, sin, sattn, su,
        sgain, token_ids.reshape(8, 128), row_order.reshape(128, 128),
    )
    return weight, gain.reshape(512)


def solution(mesh):
    placed = (
        P("student", "teacher"),
        P("student", "teacher"),
        P("student", "teacher"),
        P("teacher"),
        P("teacher", "student"),
        P("student", "teacher"),
        P("student", "teacher"),
        P("student", "teacher"),
        P("teacher"),
        P("student"),
        P(),
    )
    return jax.shard_map(
        step,
        mesh=mesh,
        in_specs=placed,
        out_specs=(P("student", "teacher"), P("teacher")),
        check_vma=False,
    )
```

```python
import math

import jax
import jax.numpy as jnp
from jax import lax
from jax.experimental import pallas as pl
from jax.experimental.pallas import tpu as pltpu
from jax.sharding import PartitionSpec as P

DT = 8192
DS = 4096
PAD_ID = 128004
epsilon = 1e-05

BF = jnp.bfloat16
F32 = jnp.float32
SLOTS = 256
LOSS = 1.0 / math.sqrt(16384)


def div(a, b):
    return lax.div(a, jnp.int32(b))


def rem(a, b):
    return lax.rem(a, jnp.int32(b))


class Place:
    def __init__(self):
        t = lax.axis_index("teacher")
        s = lax.axis_index("student")
        self.t, self.s = t, s
        self.zh, self.y = div(t, 4), rem(t, 4)
        self.zl, self.x, self.core = div(s, 8), rem(div(s, 2), 4), rem(s, 2)
        self.z = self.zh * 2 + self.zl

    def dev(self, dz=0, dy=0, dx=0, dc=0):
        t, s = self.index(dz, dy, dx, dc)
        return {"teacher": t, "student": s}

    def index(self, dz=0, dy=0, dx=0, dc=0):
        z, y, x, c = self.z, self.y, self.x, self.core
        if dz:
            z = rem(z + (dz % 4), 4)
        if dy:
            y = rem(y + (dy % 4), 4)
        if dx:
            x = rem(x + (dx % 4), 4)
        if dc:
            c = 1 - c
        return div(z, 2) * 4 + y, rem(z, 2) * 8 + x * 2 + c


class Net:
    def __init__(self, send, recv):
        self.send, self.recv, self.n, self.open = send, recv, 0, []

    def copy(self, src, dst, device):
        c = pltpu.make_async_remote_copy(
            src_ref=src,
            dst_ref=dst,
            send_sem=self.send.at[self.n],
            recv_sem=self.recv.at[self.n],
            device_id=device,
            device_id_type=pl.DeviceIdType.MESH,
        )
        self.n += 1
        c.start()
        self.open.append(c)
        return c

    def sent(self, copies):
        for c in copies:
            c.wait_send()
        gone = {id(c) for c in copies}
        self.open = [c for c in self.open if id(c) not in gone]

    def finish(self):
        for c in self.open:
            c.wait_send()
        self.open = []


def got(*copies):
    for c in copies:
        c.wait_recv()


def to_rows(lanes, out):
    for q in range(8):
        turned = jnp.transpose(lanes[q * 128 : q * 128 + 128, :])
        out[q : q + 1, :] = jnp.sum(turned, axis=0, keepdims=True)


def to_columns(rows, out):
    for q in range(8):
        wide = jnp.broadcast_to(rows[q : q + 1, :], (128, 128))
        out[q * 128 : q * 128 + 128, :] = jnp.transpose(wide)


def fold(a):
    return a[:, 0:128] + a[:, 128:256] + a[:, 256:384] + a[:, 384:512]


def step_kernel(
    tin, tattn, tw, tgain_in, proj, sin, sattn, su, sgain_in, tokens, order_in,
    grecv, gains,
    bufA, bufC, bufW, bufP, bufU, tinv, sinv, hid,
    pick, tmpA, tmpC, tmpD, tmpE, tmpZ, rz, r1, r2, b1, b2, r3, zs,
    sq_out, sres_out, ssq_out, target, frecv, gn, sibr, tok, rowbuf,
    tgain, sgain, order, scol, lcol, stage, exch, gstage,
    send, recv, local,
):
    p = Place()
    up, down = {"dy": 1}, {"dy": -1}
    barrier = pltpu.get_barrier_semaphore()
    teachers = [{"teacher": rem(p.t + j, 8), "student": p.s} for j in range(1, 8)]
    students = [{"teacher": p.t, "student": rem(p.s + j, 16)} for j in range(1, 16)]
    across = {"teacher": rem(p.t + 4, 8), "student": rem(p.s + 8, 16)}
    met = teachers + students + [across]
    for d in met:
        pl.semaphore_signal(barrier, inc=1, device_id=d, device_id_type=pl.DeviceIdType.MESH)
    pl.semaphore_wait(barrier, len(met))
    net = Net(send, recv)

    A = (tattn, bufA, tmpA, pl.ds(0, 512), 512)
    C = (sattn, bufC, tmpC, pl.ds(0, 128), 512)
    D = (sattn, bufC, tmpD, pl.ds(128, 128), 512)
    W = (tw, bufW, None, pl.ds(0, 1024), 128)
    Q = (proj, bufP, None, pl.ds(0, 256), 512)
    U = (su, bufU, None, pl.ds(0, 512), 64)

    def own(arr, h):
        half = arr[-1]
        return arr[0].at[pl.ds(h * half, half), arr[3]]

    def slot(arr, i, h):
        half = arr[-1]
        return arr[1].at[i, pl.ds(h * half, half), arr[3]]

    tp = p.index(dz=2)[0]
    zpart = {"teacher": p.t, "student": rem(p.s + 8, 16)}
    sp = rem(p.s + 8, 16)
    sib = p.dev(dc=1)
    sib_index = p.index(dc=1)[1]
    locals_ = []

    def bring(src, dst):
        c = pltpu.make_async_copy(src, dst, local.at[len(locals_)])
        c.start()
        locals_.append(c)
        return c

    def t_own(arr):
        ups = [net.copy(own(arr, h), slot(arr, p.t, h), p.dev(dy=1)) for h in (0, 1)]
        downs = [net.copy(own(arr, h), slot(arr, p.t, h), p.dev(dy=-1)) for h in (1, 0)][::-1]
        return ups, downs

    def t_hop1(arr):
        return [
            net.copy(own(arr, 0), arr[2].at[0], p.dev(dz=1)),
            net.copy(own(arr, 1), arr[2].at[1], p.dev(dz=-1)),
        ]

    def t_hop2(arr, hop1):
        got(hop1[0])
        a = net.copy(arr[2].at[0], slot(arr, p.index(dz=-1)[0], 0), p.dev(dz=1))
        got(hop1[1])
        b = net.copy(arr[2].at[1], slot(arr, p.index(dz=1)[0], 1), p.dev(dz=-1))
        return [a, b]

    def t_forward(arr, ups, downs, dz):
        got(ups[0])
        a = net.copy(slot(arr, p.index(dz=dz, dy=-1)[0], 0), slot(arr, p.index(dz=dz, dy=-1)[0], 0), p.dev(dy=1))
        got(downs[1])
        b = net.copy(slot(arr, p.index(dz=dz, dy=1)[0], 1), slot(arr, p.index(dz=dz, dy=1)[0], 1), p.dev(dy=-1))
        return [a, b]

    def t_partner(arr, hop2):
        got(*hop2)
        ups = [net.copy(slot(arr, tp, h), slot(arr, tp, h), p.dev(dy=1)) for h in (0, 1)]
        downs = [net.copy(slot(arr, tp, h), slot(arr, tp, h), p.dev(dy=-1)) for h in (1, 0)][::-1]
        return ups, downs

    def d_hop1(dy, halves=(0, 1)):
        out = []
        for h in halves:
            src = own(D, h) if dy == 0 else slot(D, p.index(dy=dy)[0], h)
            out.append(net.copy(src, tmpD.at[dy % 4, h], p.dev(dz=(1, -1)[h])))
        return out

    def d_hop2(dy, hop1):
        out = []
        for h, c in enumerate(hop1):
            got(c)
            at = slot(D, p.index(dz=(-1, 1)[h], dy=dy)[0], h)
            out.append(net.copy(tmpD.at[dy % 4, h], at, p.dev(dz=(1, -1)[h])))
        return out

    def s_own(arr):
        ups = [net.copy(own(arr, h), slot(arr, p.s, h), p.dev(dx=1)) for h in (0, 1)]
        downs = [net.copy(own(arr, h), slot(arr, p.s, h), p.dev(dx=-1)) for h in (1, 0)][::-1]
        return ups, downs

    def s_side(arr):
        return net.copy(arr[0], arr[1].at[p.s], zpart)

    def s_partner(arr, side):
        got(side)
        ups = [net.copy(slot(arr, sp, h), slot(arr, sp, h), p.dev(dx=1)) for h in (0, 1)]
        downs = [net.copy(slot(arr, sp, h), slot(arr, sp, h), p.dev(dx=-1)) for h in (1, 0)][::-1]
        return ups, downs

    def s_index(dx, other):
        i = p.index(dx=dx)[1]
        return rem(i + 8, 16) if other else i

    def s_forward(arr, ups, downs, other):
        got(ups[0])
        i = s_index(-1, other)
        a = net.copy(slot(arr, i, 0), slot(arr, i, 0), p.dev(dx=1))
        got(downs[1])
        j = s_index(1, other)
        b = net.copy(slot(arr, j, 1), slot(arr, j, 1), p.dev(dx=-1))
        return [a, b]

    def share(arr, i):
        return net.copy(arr[1].at[i], arr[1].at[i], sib)

    ssides, sowns, shared = {}, {}, []
    aown = t_own(A)
    ahop1 = t_hop1(A)
    for n, arr in (("W", W), ("Q", Q)):
        sowns[n] = s_own(arr)
        if n == "W":
            ssides[n] = s_side(arr)
        shared.append(net.copy(arr[0], arr[1].at[p.s], sib))
    bring(tattn, bufA.at[p.t])
    bring(tw, bufW.at[p.s])
    bring(proj, bufP.at[p.s])
    bring(tin, tinv)
    bring(sattn, bufC.at[p.t])
    bring(su, bufU.at[p.s])
    bring(sin, sinv)
    down_ = t_own(D)
    told = [net.copy(tokens, tok.at[p.s], d) for d in students]
    bring(tokens, tok.at[p.s])
    bring(tgain_in, tgain)
    bring(sgain_in, sgain)
    bring(order_in, order)
    sowns["U"] = s_own(U)
    shared.append(net.copy(U[0], U[1].at[p.s], sib))
    S = (("W", W), ("Q", Q), ("U", U))
    sfwd, sfwd2, sparts = {}, {}, {}

    ahop2 = t_hop2(A, ahop1)
    dhop1, dhop2 = {}, {}
    ssides["Q"] = s_side(Q)
    dhop1[0] = d_hop1(0)
    ssides["U"] = s_side(U)
    for n, arr in S[:2]:
        sfwd[n] = s_forward(arr, *sowns[n], False)
    afwd = t_forward(A, *aown, 0)
    sparts["W"] = s_partner(W, ssides["W"])
    dfwd = t_forward(D, *down_, 0)
    apart = t_partner(A, ahop2)
    got(down_[0][1], down_[1][0])
    dhop1[-1] = d_hop1(-1)
    dhop1[1] = d_hop1(1)
    dhop2[0] = d_hop2(0, dhop1[0])
    sparts["Q"] = s_partner(Q, ssides["Q"])
    for n, arr in S[:2]:
        got(sowns[n][0][1], sowns[n][1][0])
        shared.append(share(arr, sp))
        shared.append(share(arr, s_index(-1, False)))
        shared.append(share(arr, s_index(1, False)))
    sfwd["U"] = s_forward(U, *sowns["U"], False)
    sparts["U"] = s_partner(U, ssides["U"])
    dhop2[-1] = d_hop2(-1, dhop1[-1])
    dhop2[1] = d_hop2(1, dhop1[1])
    for n, arr in S[:2]:
        sfwd2[n] = s_forward(arr, *sparts[n], True)
    afwd2 = t_forward(A, *apart, 2)
    chop1 = t_hop1(C)
    got(*dfwd)
    dhop1[2] = d_hop1(2)
    cown = t_own(C)
    chop2 = t_hop2(C, chop1)
    dhop2[2] = d_hop2(2, dhop1[2])
    for n, arr in S[:2]:
        got(*sfwd[n], sparts[n][0][1], sparts[n][1][0])
        shared.append(share(arr, s_index(2, False)))
        shared.append(share(arr, s_index(-1, True)))
        shared.append(share(arr, s_index(1, True)))
    sfwd2["U"] = s_forward(U, *sparts["U"], True)
    got(sowns["U"][0][1], sowns["U"][1][0], sparts["U"][0][1], sparts["U"][1][0], *sfwd["U"])
    ushared = [
        share(U, sp),
        share(U, s_index(-1, False)),
        share(U, s_index(1, False)),
        share(U, s_index(2, False)),
        share(U, s_index(-1, True)),
        share(U, s_index(1, True)),
    ]
    for c in locals_:
        c.wait()

    wide = lax.broadcasted_iota(jnp.int32, (64, 1024), 1).astype(F32)
    narrow = lax.broadcasted_iota(jnp.int32, (64, 128), 1).astype(F32)
    rowbuf[...] = jnp.zeros_like(rowbuf)
    for m in range(16):
        b = rem(p.s + m, 16)
        rowbuf[0, m : m + 1, :] = order[pl.ds(b * 8 + div(p.s, 2), 1), :].astype(F32)
    rowbuf[1, 0:8, :] = order[pl.ds(pl.multiple_of(p.s * 8, 8), 8), :].astype(F32)
    for n in range(2):
        rowbuf[2 + n] = jnp.transpose(rowbuf[n])
    half = pl.ds(pl.multiple_of(rem(p.s, 2) * 64, 64), 64)
    base = (p.s * 1024).astype(F32)
    mine = rowbuf[2, half, :] - base
    for m in range(16):
        pick[m * 64 : m * 64 + 64, :] = jnp.where(wide == mine[:, m : m + 1], 1.0, 0.0).astype(BF)

    got(*told)
    for b in range(16):
        low = (b % 2) * 64
        named = rowbuf[3, low : low + 64, b // 2 : b // 2 + 1] - float(b * 1024)
        live = jnp.where(tok[b] != PAD_ID, LOSS, 0.0)
        acc = jnp.zeros((64, 128), F32)
        for q in range(8):
            acc = acc + jnp.where(narrow == named - float(q * 128), live[q : q + 1, :], 0.0)
        total = jnp.sum(acc, axis=1, keepdims=True)
        lcol[b * 64 : b * 64 + 64, :] = jnp.broadcast_to(total, (64, 128))

    for n, arr in S[:2]:
        got(*sfwd2[n])
        shared.append(share(arr, s_index(2, True)))
    got(aown[0][1], aown[1][0], *afwd, apart[0][1], apart[1][0], *afwd2)
    cfwd = t_forward(C, *cown, 0)
    cpart = t_partner(C, chop2)
    got(*shared)
    sq_out[...] = jnp.zeros_like(sq_out)

    def first(i, carry):
        rows = pl.ds(pl.multiple_of(div(i, 2) * 512, 512), 512)
        cols = pl.ds(pl.multiple_of(rem(i, 2) * 512, 512), 512)
        acc = tinv[rows, cols].astype(F32)
        for t in range(8):
            w = bufW[2 * t : 2 * t + 2, :, cols].reshape(512, 512)
            acc = acc + jnp.dot(bufA[t, rows, :], w, preferred_element_type=F32)
        square = acc * acc
        sq_out[rows, :] += square[:, 0:128] + square[:, 128:256] + square[:, 256:384] + square[:, 384:512]
        hid[rows, cols] = (acc * tgain[cols].astype(F32).reshape(1, 512)).astype(BF)
        return carry

    lax.fori_loop(0, 2, first, 0)
    cfwd2 = t_forward(C, *cpart, 2)
    lax.fori_loop(2, 4, first, 0)
    early = list(net.open)
    a_sends = [*aown[0], *aown[1], *ahop1, *ahop2, *afwd, *apart[0], *apart[1], *afwd2]
    net.sent(a_sends)
    gone = {id(c) for c in a_sends}
    early = [c for c in early if id(c) not in gone]

    def columns(half):
        return pl.ds(half * 256, 256)

    def project(k, half):
        def step(i, carry):
            rows = pl.ds(pl.multiple_of(i * 512, 512), 512)
            bufA[k, rows, columns(half)] = jnp.dot(
                hid[rows, :], bufP[2 * k + half], preferred_element_type=F32
            ).astype(BF)
            return carry

        lax.fori_loop(0, 2, step, 0)

    def block(far, dy):
        zh = 1 - p.zh if far else p.zh
        y = rem(p.y + (dy % 4), 4)
        return zh * 4 + y

    lo, hi = pl.ds(0, 512), pl.ds(512, 512)
    right = pl.ds(512, 512)

    def add(k, half, base, count, ref, rebase):
        def step(i, carry):
            at = pl.ds(pl.multiple_of(rebase + i * 128, 128), 128)
            rows = pl.ds(pl.multiple_of(base + i * 128, 128), 128)
            both = bufA[k, rows, columns(half)].astype(F32) + ref[at, :].astype(F32)
            bufA[k, rows, columns(half)] = both.astype(BF)
            return carry

        lax.fori_loop(0, count, step, 0)

    def piece(k, half, rows):
        return bufA.at[k, rows, columns(half)]

    def open_to(k, half, dst):
        return (
            net.copy(piece(k, half, lo), dst.at[0], p.dev(dy=1)),
            net.copy(piece(k, half, hi), dst.at[1], p.dev(dy=-1)),
        )

    def added(far, half, opened, src, dst):
        ku, kd = block(far, 1), block(far, -1)
        got(opened[0])
        add(ku, half, 0, 4, src.at[0], 0)
        u = net.copy(piece(ku, half, lo), dst.at[0, lo, :], p.dev(dy=1))
        got(opened[1])
        add(kd, half, 512, 4, src.at[1], 0)
        d = net.copy(piece(kd, half, hi), dst.at[1, hi, :], p.dev(dy=-1))
        return u, d

    def plain_up(far, half, dst):
        return net.copy(piece(block(far, 1), half, hi), dst.at[0, hi, :], p.dev(dy=1))

    def plain_down(far, half, dst):
        return net.copy(piece(block(far, -1), half, lo), dst.at[1, lo, :], p.dev(dy=-1))

    z1, z2 = {}, {}

    def z_first(dy):
        k = block(True, dy)
        project(k, 1)
        z1[dy] = (
            net.copy(piece(k, 1, lo), tmpZ.at[dy % 4, 0], p.dev(dz=1)),
            net.copy(piece(k, 1, hi), tmpZ.at[dy % 4, 1], p.dev(dz=-1)),
        )

    def z_on(dy):
        got(z1[dy][0])
        a = net.copy(tmpZ.at[dy % 4, 0], rz.at[dy % 4, lo, :], p.dev(dz=1))
        got(z1[dy][1])
        b = net.copy(tmpZ.at[dy % 4, 1], rz.at[dy % 4, hi, :], p.dev(dz=-1))
        z2[dy] = (a, b)

    def z_add(dy):
        got(*z2[dy])
        add(block(False, dy), 1, 0, 8, rz.at[dy % 4], 0)

    def exchange(kind):
        return [net.copy(stage.at[kind], exch.at[kind, p.t], d) for d in teachers]

    def exchanged(kind, copies):
        exch[kind, p.t] = stage[kind]
        got(*copies)
        total = exch[kind, 0]
        for t in range(1, 8):
            total = total + exch[kind, t]
        return total

    z_first(2)
    project(block(True, 2), 0)
    open_far = open_to(block(True, 2), 0, r1.at[0])
    z_first(1)
    project(block(True, 1), 0)
    up_far = plain_up(True, 0, r2.at[0])
    project(block(True, -1), 0)
    down_far = plain_down(True, 0, r2.at[0])
    project(block(False, 2), 0)
    open_near = open_to(block(False, 2), 0, r1.at[1])
    z_on(2)
    z_first(-1)
    added_far = added(True, 0, open_far, r1.at[0], r2.at[0])
    z_on(1)
    project(block(False, 1), 0)
    up_near = plain_up(False, 0, r2.at[1])
    project(block(False, -1), 0)
    down_near = plain_down(False, 0, r2.at[1])
    for dy in (2, 1, -1, 0):
        project(block(False, dy), 1)
    k_far, k_near = block(True, 0), block(False, 0)
    project(k_far, 0)
    project(k_near, 0)
    z_on(-1)
    z_first(0)
    z_add(2)
    opened = open_to(block(False, 2), 1, b1)
    added_near = added(False, 0, open_near, r1.at[1], r2.at[1])
    got(cown[0][1], cown[1][0], *cfwd, cpart[0][1], cpart[1][0], *cfwd2)
    got(*dhop2[0], *dhop2[1], *dhop2[-1], *dhop2[2])
    got(*sfwd2["U"])
    ushared.append(share(U, s_index(2, True)))
    got(*ushared)

    def student(i, carry):
        rows = pl.ds(pl.multiple_of(i * 512, 512), 512)
        acc = sinv[rows, :].astype(F32)
        for t in range(8):
            w = bufU[2 * t : 2 * t + 2].reshape(256, 512)
            acc = acc + jnp.dot(bufC[t, rows, :], w, preferred_element_type=F32)
        ssq_out[rows, :] = fold(acc * acc)
        sres_out[rows, :] = acc
        return carry

    lax.fori_loop(0, 2, student, 0)
    to_rows(ssq_out, stage.at[1])
    ssums = exchange(1)

    net.sent(early)

    def turn(i, carry):
        t = div(i, 8)
        rows = pl.ds(pl.multiple_of(rem(i, 8) * 128, 128), 128)
        block = bufC[t, rows, :].astype(F32)
        at = pl.ds(pl.multiple_of(rem(t, 2) * 128, 128), 128)
        for core in range(2):
            turned = jnp.transpose(block[:, core * 128 : core * 128 + 128])
            bufW[core * 4 + div(t, 2), at, rows] = turned.astype(BF)
        return carry

    lax.fori_loop(0, 16, turn, 0)

    def three(k, half, src, i):
        at = pl.ds(pl.multiple_of(i * 128, 128), 128)
        own_part = bufA[k, at, columns(half)].astype(F32)
        return at, own_part + src[0, at, :].astype(F32) + src[1, at, :].astype(F32)

    z_add(1)
    up_last = plain_up(False, 1, b2)
    got(up_far, down_far, *added_far)

    def far_sum(i, carry):
        at, total = three(k_far, 0, r2.at[0], i)
        zs[at, columns(0)] = total.astype(BF)
        return carry

    lax.fori_loop(0, 8, far_sum, 0)
    hop1 = (
        net.copy(zs.at[lo, columns(0)], tmpE.at[0], p.dev(dz=1)),
        net.copy(zs.at[hi, columns(0)], tmpE.at[1], p.dev(dz=-1)),
    )
    z_on(0)
    to_rows(sq_out, stage.at[0])
    tsums = exchange(0)
    lax.fori_loop(16, 32, turn, 0)
    got(hop1[0])
    h2a = net.copy(tmpE.at[0], r3.at[lo, :], p.dev(dz=1))
    got(hop1[1])
    h2b = net.copy(tmpE.at[1], r3.at[hi, :], p.dev(dz=-1))
    z_add(-1)
    down_last = plain_down(False, 1, b2)
    added_last = added(False, 1, opened, b1, b2)
    lax.fori_loop(32, 48, turn, 0)
    to_columns(lax.rsqrt(exchanged(0, tsums) / DT + epsilon), sq_out)
    to_columns(lax.rsqrt(exchanged(1, ssums) / DS + epsilon), scol)
    got(up_near, down_near, *added_near)
    lax.fori_loop(48, 64, turn, 0)
    got(h2a, h2b)

    def near_sum(i, carry):
        at, total = three(k_near, 0, r2.at[1], i)
        total = total + r3[at, :].astype(F32)
        target[at, columns(0)] = (total * sq_out[at, 0:1]).astype(BF)
        return carry

    lax.fori_loop(0, 8, near_sum, 0)

    def send_rows(half):
        out = {}
        for group in (1, 2, 3, 0):
            rows = slice(group * 256, group * 256 + 256)
            picked = jnp.dot(
                pick[rows, :], target[:, columns(half)], preferred_element_type=F32
            ).astype(BF)
            tinv[rows, columns(half)] = picked
            if group == 0:
                frecv[p.s, :, columns(half)] = picked[0:64, :]
            for m in range(max(group * 4, 1), group * 4 + 4):
                out[m] = net.copy(
                    tinv.at[pl.ds(m * 64, 64), columns(half)],
                    frecv.at[p.s, :, columns(half)],
                    students[m - 1],
                )
        return out

    moved = send_rows(0)
    z_add(0)
    got(up_last, down_last, *added_last)

    def last_sum(i, carry):
        at, total = three(k_near, 1, b2, i)
        target[at, columns(1)] = (total * sq_out[at, 0:1]).astype(BF)
        return carry

    lax.fori_loop(0, 8, last_sum, 0)
    moved_last = send_rows(1)

    def compared(half, copies):
        cols = columns(half)
        gain_values = sgain[cols].astype(F32).reshape(1, 256)
        partial = jnp.zeros((1, 256), F32)
        for m in (0, *range(4, 16), 1, 2, 3):
            if m:
                got(copies[m])
            b = rem(p.s + (16 - m), 16)
            rows = pl.ds(pl.multiple_of(b * 64, 64), 64)
            normed = sres_out[rows, cols] * scol[rows, 0:1]
            grad_out = (normed * gain_values - frecv[b, :, cols].astype(F32)) * lcol[rows, 0:1]
            partial = partial + jnp.sum(grad_out * normed, axis=0, keepdims=True)
            grad_norm = grad_out * gain_values
            gn[rows, cols] = grad_norm
            product = grad_norm * normed
            lanes = product[:, 0:128] + product[:, 128:256]
            ssq_out[rows, :] = lanes if half == 0 else ssq_out[rows, :] + lanes
        gstage[:, cols] = partial

    compared(0, moved)
    compared(1, moved_last)
    to_rows(ssq_out, stage.at[2])
    inner = exchange(2)
    gained = [net.copy(gstage, gains.at[p.s], d) for d in students]
    net.sent(hop1)
    to_columns(exchanged(2, inner) / DS, sq_out)

    def grad(i, carry):
        rows = pl.ds(pl.multiple_of(i * 128, 128), 128)
        scale = scol[rows, 0:1]
        normed = sres_out[rows, :] * scale
        zs[rows, :] = (scale * (gn[rows, :] - normed * sq_out[rows, 0:1])).astype(BF)
        return carry

    lax.fori_loop(0, 8, grad, 0)

    def product(core, i):
        return jnp.dot(bufW[core * 4 + i], zs[...], preferred_element_type=F32)

    halves = {}
    for j in (2, 3, 1, 0):
        i = rem(div(p.s, 4) + j, 4)
        part = pl.ds(pl.multiple_of(i * 256, 256), 256)
        sinv[part, :] = product(1 - p.core, i).astype(BF)
        halves[j] = net.copy(sinv.at[part, :], sibr.at[part, :], sib)
    chip = div(p.s, 2)
    parts = []
    for j in (2, 3, 1, 0):
        i = rem(div(chip, 2) + j, 4)
        own_part = product(p.core, i)
        rows = pl.ds(pl.multiple_of(i * 256, 256), 256)
        got(halves[j])
        total = own_part + sibr[rows, :].astype(F32)
        tinv[rows, 512:1024] = total.astype(BF)
        for n in range(2):
            if j == 0 and n == 1:
                continue
            if j == 0:
                q = i * 2 + 1 - rem(chip, 2)
            else:
                q = i * 2 + rem(chip + n, 2)
            sub_rows = pl.ds(pl.multiple_of(q * 128, 128), 128)
            to = {"teacher": p.t, "student": q * 2 + p.core}
            parts.append(net.copy(tinv.at[sub_rows, right], grecv.at[len(parts)], to))
    last = [
        bring(gstage, gains.at[p.s]),
        bring(tinv.at[pl.ds(pl.multiple_of(chip * 128, 128), 128), right], grecv.at[7]),
    ]
    for c in last:
        c.wait()
    got(*gained, *parts)
    net.finish()


def step(tin, tattn, tw, tgain, proj, sin, sattn, su, sgain, token_ids, row_order):
    anywhere = pl.BlockSpec(memory_space=pl.ANY)
    V = pltpu.VMEM
    parts, gains = pl.pallas_call(
        step_kernel,
        out_shape=(
            jax.ShapeDtypeStruct((8, 128, 512), BF),
            jax.ShapeDtypeStruct((16, 1, 512), F32),
        ),
        in_specs=[anywhere] * 11,
        out_specs=(anywhere, anywhere),
        scratch_shapes=[
            V((8, 1024, 512), BF),
            V((8, 1024, 256), BF),
            V((16, 256, 1024), BF),
            V((16, 1024, 256), BF),
            V((16, 128, 512), BF),
            V((1024, 1024), BF),
            V((1024, 512), BF),
            V((1024, 1024), BF),
            V((1024, 1024), BF),
            V((2, 512, 512), BF),
            V((2, 512, 128), BF),
            V((4, 2, 512, 128), BF),
            V((2, 512, 256), BF),
            V((4, 2, 512, 256), BF),
            V((4, 1024, 256), BF),
            V((2, 2, 512, 256), BF),
            V((2, 2, 1024, 256), BF),
            V((2, 512, 256), BF),
            V((2, 1024, 256), BF),
            V((1024, 256), BF),
            V((1024, 512), BF),
            V((1024, 128), F32),
            V((1024, 512), F32),
            V((1024, 128), F32),
            V((1024, 512), BF),
            V((16, 64, 512), BF),
            V((1024, 512), F32),
            V((1024, 512), BF),
            V((16, 8, 128), jnp.int32),
            V((4, 128, 128), F32),
            V((1024,), BF),
            V((512,), BF),
            V((128, 128), jnp.int32),
            V((1024, 128), F32),
            V((1024, 128), F32),
            V((3, 8, 128), F32),
            V((3, 8, 8, 128), F32),
            V((1, 512), F32),
            pltpu.SemaphoreType.DMA((SLOTS,)),
            pltpu.SemaphoreType.DMA((SLOTS,)),
            pltpu.SemaphoreType.DMA((16,)),
        ],
        compiler_params=pltpu.CompilerParams(
            collective_id=0, has_side_effects=True, vmem_limit_bytes=67043328
        ),
        name="step",
    )(
        tin, tattn, tw, tgain, proj, sin, sattn, su,
        sgain, token_ids.reshape(8, 128), row_order.reshape(128, 128),
    )
    return jnp.sum(parts.astype(F32), axis=0), jnp.sum(gains, axis=(0, 1))


def solution(mesh):
    placed = (
        P("student", "teacher"),
        P("student", "teacher"),
        P("student", "teacher"),
        P("teacher"),
        P("teacher", "student"),
        P("student", "teacher"),
        P("student", "teacher"),
        P("student", "teacher"),
        P("teacher"),
        P("student"),
        P(),
    )
    return jax.shard_map(
        step,
        mesh=mesh,
        in_specs=placed,
        out_specs=(P("student", "teacher"), P("teacher")),
        check_vma=False,
    )
```
